32 devices in a mesh: region: 16 (over z, y, x), member: 2 (over core).
Axes of the slice: x: 2, y: 2, z: 4, core: 2. Of those that a mesh axis runs over, the one named last changes fastest.
Arguments:
- perturbations: bfloat16 [80, 2, 64, 2048], P('member', None, None, 'region'), may hold values from -0.65625 to 0.65625
- control: float32 [80, 64, 2048], P('member', None, 'region'), may hold values from -6 to 6
- vertical_loc: bfloat16 [64, 64], replicated, may hold values from -0.75 to 0.75
- block_kernels: bfloat16 [4, 128, 128], replicated, may hold values from -0.3125 to 0.3125
- loc_pattern: int32 [16, 3], replicated, may hold values from 0 to 3
- obs_region: int32 [16384, 1], P('region'), may hold values from 0 to 15; in each aligned block of 512 rows (0 to 511, 512 to 1023, ...) at most 64 rows name the same one
- obs_slot: int32 [16384], P('region'), may hold values from 0 to 1
- obs_cell: int32 [16384], P('region'), may hold values from 0 to 127
- innovations: float32 [64, 16384], P(None, 'region'), may hold values from -12 to 12
- obs_weight: float32 [128, 128, 128], P('region'), may hold values from -0.0375 to 2, as said below
Outputs:
- analysis: float32 [80, 64, 2048], P('member', None, 'region')
The draws below stay inside these ranges and needn't reach their ends.
Inputs may be any that keep to these rules, and one draw needn't show every extreme that they name: `obs_region`: in each aligned block of 512 rows, no region is named by more than 64 rows. `obs_weight`: each tile is symmetric, and in each row the diagonal entry exceeds the sum of the magnitudes of the other entries.
All inputs are finite; a program needn't handle non-finite values.
Results may differ from the reference program's by a relative error of at most 0.013.
Values may be sent and summed in bfloat16 or wider, within the bound.
No kernel may reach another device: no remote copies, remote signals or barrier semaphores. Data moves between devices by JAX's collectives and lax.ppermute only.
A program may use at most 64 MiB of HBM per device.

```python
import math
import jax
import jax.numpy as jnp
import numpy as np
from jax import lax

LEV = 64
MEMBERS = 80
SLOTS = 2
BLOCK = 128
TILE = 128
KTYPES = 4
ITERS = 2
CELLS_DEV = 128
OBS_DEV = 1024
REGIONS = 16
NCELLS = 2048
NBLOCKS = 16
OBS = 16384
TILES = 128
OBS_GROUP = 512
CAP = 64


def draw_innovations(key, part):
    columns = jnp.arange(OBS, dtype=jnp.int32)
    region_share = (columns // OBS_DEV).astype(jnp.float32) / max(REGIONS - 1, 1)
    scaling = 1.0 + 2.0 * region_share
    values = jnp.clip(jax.random.normal(key, (LEV, OBS), jnp.float32), -4.0, 4.0)
    return values * scaling[None, :]


def draw_obs_weight(key, part):
    key_diag = jax.random.fold_in(key, 11)
    key_off = jax.random.fold_in(key, 13)
    diagonal = jax.random.uniform(key_diag, (TILES, TILE), jnp.float32, 1.0, 2.0)
    raw_values = jax.random.uniform(key_off, (TILES, TILE, TILE), jnp.float32, -1.0, 1.0)
    mixed = 0.5 * (raw_values + jnp.swapaxes(raw_values, 1, 2))
    indices = jnp.arange(TILE, dtype=jnp.int32)
    spacing = jnp.abs(indices[:, None] - indices[None, :]).astype(jnp.float32)
    falloff = jnp.where(spacing > 0.0, jnp.exp(-spacing / 8.0), 0.0)
    identity = jnp.where(spacing > 0.0, 0.0, 1.0)
    return diagonal[:, :, None] * identity[None] + 0.0375 * mixed * falloff[None]


def touch_ends(drawn, rng, least, high):
    longest = drawn.shape.index(max(drawn.shape))
    spots = []
    for shift in (0, 1):
        where = [jax.random.randint(jax.random.fold_in(rng, axis), (), 0, length) for axis, length in enumerate(drawn.shape)]
        where[longest] = (where[longest] + shift) % drawn.shape[longest]
        spots.append(tuple(where))
    return drawn.at[spots[0]].set(least).at[spots[1]].set(high)


def steps_of(stream_key, shape, split, smallest, largest):
    def one(dim, parts):
        steps = jax.random.uniform(jax.random.fold_in(jax.random.fold_in(stream_key, 6), dim), (parts,), jnp.float32, smallest / len(split), largest / len(split))
        return jnp.repeat(jnp.exp(steps), shape[dim] // parts).reshape((-1,) + (1,) * (len(shape) - dim - 1))

    gain = one(*split[0])
    for cut in split[1:]:
        gain = gain * one(*cut)
    return gain


def assign_block(key, own, number, rows, count, top, most, slope):
    order = jax.random.permutation(key, count)
    packed, usual = shares(count, rows * top, most, slope, True), shares(count, rows * top, most, slope, False)
    places = jnp.arange(count)

    def named(lengths, rotation):
        used = int((lengths > 0).sum())
        fixed = max(1, used // 4)
        shifted = fixed + (places - fixed + rotation * (used - fixed)) % max(1, count - fixed)
        return jnp.zeros((count,), jnp.int32).at[order[jnp.where(places < fixed, places, shifted)]].set(jnp.asarray(lengths, jnp.int32))

    lengths = jnp.where(number % 4 == 0, named(packed, number // 4), named(usual, number - number // 4 - 1))
    mixed = jax.random.permutation(jax.random.fold_in(own, 3), count)
    donor, sink = mixed[0:count // 2 * 2:2], mixed[1:count // 2 * 2:2]
    room = jnp.minimum(lengths[donor] - 1, most - lengths[sink]) // 2
    room = jnp.where((donor == order[0]) | (sink == order[0]) | (lengths[sink] == 0), 0, jnp.maximum(room, 0))
    shifted = jax.random.randint(jax.random.fold_in(own, 4), (count // 2,), 0, 1 << 20) % (room + 1)
    lengths = lengths.at[donor].add(-shifted).at[sink].add(shifted)
    items = jnp.searchsorted(jnp.cumsum(lengths), jnp.arange(rows * top), side="right").astype(jnp.int32)
    listing = items.reshape(top, rows).T
    listing = listing[jax.random.permutation(jax.random.fold_in(own, 1), rows)]
    rotation = jax.random.randint(jax.random.fold_in(own, 2), (rows, 1), 0, top)
    return jnp.take_along_axis(listing, (jnp.arange(top)[None, :] + rotation) % top, axis=1)


def shares(count, total, most, slope, full):
    loads = [(1 << 20) // math.isqrt(standing ** slope) + 1 for standing in range(1, count + 1)]
    largest = most if full else min(most, max(-(-total // count), total * loads[0] // sum(loads)))
    least = 1 if total - largest >= count - 1 else 0
    given, spare = [largest] + [least] * (count - 1), total - largest - least * (count - 1)
    while spare > 0:
        free = [i for i in range(1, count) if given[i] < largest] or [i for i in range(1, count) if given[i] < most]
        whole, left = sum([loads[i] for i in free]), spare
        for i in free:
            extra = min(most - given[i], max(1, left * loads[i] // whole), spare)
            given[i] = given[i] + extra
            spare = spare - extra
    return np.array(given)


def scatter_about(rng, shape, scale, bound, cuts=(), held_as=jnp.bfloat16):
    loudness = steps_of(rng, shape, cuts, -0.22, 0.18) if cuts else 1.0
    array = jax.random.normal(rng, shape, jnp.float32) * scale * loudness
    return jnp.minimum(jnp.maximum(array, -bound), bound).astype(held_as)


def setup_inputs(seed: int = 0) -> dict:
    splits = jax.random.split(jax.random.key(seed), 11)
    perturbations = scatter_about(splits[0], (MEMBERS, SLOTS, LEV, NCELLS), 0.11, 0.65625, ((0, 2), (3, 16)))
    control = scatter_about(splits[1], (MEMBERS, LEV, NCELLS), 1.0, 6.0, ((0, 2), (2, 16)), jnp.float32)
    vertical_loc = scatter_about(splits[2], (LEV, LEV), LEV ** -0.5, 0.75)
    block_kernels = scatter_about(splits[3], (KTYPES, BLOCK, BLOCK), (3 * BLOCK) ** -0.5, 0.3125)
    loc_pattern = touch_ends(jax.random.randint(splits[4], (NBLOCKS, 3), 0, KTYPES), jax.random.fold_in(splits[4], 1), 0, KTYPES - 1).astype(jnp.int32)
    obs_region_keys = jax.random.split(jax.random.fold_in(splits[5], 1), OBS // OBS_GROUP)
    obs_region_turns = jax.random.permutation(jax.random.fold_in(splits[5], 3), OBS // OBS_GROUP)
    obs_region = jax.vmap(lambda own, number: assign_block(jax.random.fold_in(splits[5], 2), own, number, OBS_GROUP, REGIONS, 1, CAP, 2))(obs_region_keys, obs_region_turns).reshape((OBS, 1))
    obs_slot = touch_ends(jax.random.randint(splits[6], (OBS,), 0, SLOTS), jax.random.fold_in(splits[6], 1), 0, SLOTS - 1).astype(jnp.int32)
    obs_cell = touch_ends(jax.random.randint(splits[7], (OBS,), 0, CELLS_DEV), jax.random.fold_in(splits[7], 1), 0, CELLS_DEV - 1).astype(jnp.int32)
    innovations = draw_innovations(jax.random.fold_in(splits[10], 71), 0)
    obs_weight = draw_obs_weight(jax.random.fold_in(splits[10], 71), 0)
    return {"perturbations": perturbations, "control": control, "vertical_loc": vertical_loc, "block_kernels": block_kernels, "loc_pattern": loc_pattern, "obs_region": obs_region, "obs_slot": obs_slot, "obs_cell": obs_cell, "innovations": innovations, "obs_weight": obs_weight}


def horizontal(values, tables):
    padded = jnp.pad(values, ((0, 0), (BLOCK, BLOCK)))
    summed = jnp.zeros((LEV, NBLOCKS, BLOCK), jnp.float32)
    for offset in range(3):
        window = padded[:, offset * BLOCK: offset * BLOCK + NCELLS].reshape(LEV, NBLOCKS, BLOCK)
        summed = summed + jnp.einsum("lbk,bkj->lbj", window.astype(jnp.float32), tables[offset])
    return summed.reshape(LEV, NCELLS)


def horizontal_adjoint(values, tables):
    padded = jnp.pad(values, ((0, 0), (BLOCK, BLOCK)))
    summed = jnp.zeros((LEV, NBLOCKS, BLOCK), jnp.float32)
    for offset in range(3):
        first_cell = (2 - offset) * BLOCK
        window = padded[:, first_cell: first_cell + NCELLS].reshape(LEV, NBLOCKS, BLOCK)
        summed = summed + jnp.einsum("lbj,bkj->lbk", window.astype(jnp.float32), tables[offset])
    return summed.reshape(LEV, NCELLS)


def reference(perturbations, control, vertical_loc, block_kernels, loc_pattern, obs_region, obs_slot, obs_cell, innovations, obs_weight):
    pattern_pad = jnp.pad(loc_pattern, ((1, 1), (0, 0)))
    forward_tables = [block_kernels[loc_pattern[:, offset]].astype(jnp.float32) for offset in range(3)]
    backward_tables = [block_kernels[pattern_pad[2 - offset: 2 - offset + NBLOCKS, offset]].astype(jnp.float32) for offset in range(3)]
    obs_codes = (obs_slot * NCELLS + obs_region[:, 0] * CELLS_DEV + obs_cell).astype(jnp.int32)

    def apply_operator(vector, with_innovation):
        def forward_member(running, inputs):
            member_vector, member_pert = inputs
            spread = horizontal(member_vector.astype(jnp.bfloat16), forward_tables).astype(jnp.bfloat16)
            weights = jnp.dot(vertical_loc, spread, preferred_element_type=jnp.float32)
            return running + member_pert.astype(jnp.float32) * weights[None], None

        increment, _ = lax.scan(forward_member, jnp.zeros((SLOTS, LEV, NCELLS), jnp.float32), (vector, perturbations))
        flattened = increment.transpose(1, 0, 2).reshape(LEV, SLOTS * NCELLS)
        departures = flattened[:, obs_codes]
        if with_innovation:
            departures = departures - innovations
        weighted = jnp.einsum("ltk,tkj->ltj", departures.reshape(LEV, TILES, TILE), obs_weight,
                              precision=lax.Precision.HIGHEST).reshape(LEV, OBS)
        adjoint_flat = jnp.zeros((LEV, SLOTS * NCELLS), jnp.float32).at[:, obs_codes].add(weighted)
        adjoint_field = adjoint_flat.reshape(LEV, SLOTS, NCELLS).transpose(1, 0, 2)

        def backward_member(inputs):
            member_vector, member_pert = inputs
            projected = jnp.sum(member_pert.astype(jnp.float32) * adjoint_field, axis=0).astype(jnp.bfloat16)
            lifted = jnp.dot(vertical_loc.T, projected, preferred_element_type=jnp.float32).astype(jnp.bfloat16)
            return member_vector + horizontal_adjoint(lifted, backward_tables)

        return lax.map(backward_member, (vector, perturbations))

    residual = -apply_operator(control, True)
    direction = residual
    norm_now = jnp.sum(residual * residual)
    solution = control
    for iteration in range(ITERS):
        curved = apply_operator(direction, False)
        step_size = norm_now / jnp.sum(direction * curved)
        solution = solution + step_size * direction
        if iteration + 1 < ITERS:
            residual = residual - step_size * curved
            norm_next = jnp.sum(residual * residual)
            direction = residual + (norm_next / norm_now) * direction
            norm_now = norm_next
    return solution
```

```python
import functools

import jax
import jax.numpy as jnp
import numpy as np
from jax import lax
from jax.experimental import pallas as pl
from jax.experimental.pallas import tpu as pltpu
from jax.sharding import PartitionSpec as P

SLOTS = 2
TILE = 128
CELLS = 128
ITERS = 2
CODES = SLOTS * CELLS
F32 = jnp.float32
BF16 = jnp.bfloat16
HALO_CHUNKS = 2


def near_of(r, regions):
    return r ^ 1


def far_of(r, regions):
    other = r - 1 if r % 2 == 0 else r + 1
    return other if 0 <= other < regions else None


def side(r, t, regions):
    return (r, near_of(r, regions), far_of(r, regions))[t]


def dot(a, b, dims=((1,), (0,)), precision=None):
    return lax.dot_general(a, b, (dims, ((), ())), precision=precision, preferred_element_type=F32)


def halo(chunks):
    regions = lax.axis_size("region")
    pairs = [(r, r ^ 1) for r in range(regions)]
    onward = [(r, r + 2 if r % 2 == 0 else r - 2) for r in range(regions)]
    onward = [(s, d) for s, d in onward if 0 <= d < regions]
    near = [lax.ppermute(c, "region", pairs) for c in chunks]
    far = [lax.ppermute(c, "region", onward) for c in near]
    return near, far


def call(kernel, out_shape, args, scratch=()):
    return pl.pallas_call(
        kernel,
        out_shape=out_shape,
        in_specs=[pl.BlockSpec(memory_space=pltpu.VMEM)] * len(args),
        out_specs=jax.tree.map(lambda _: pl.BlockSpec(memory_space=pltpu.VMEM), out_shape),
        scratch_shapes=list(scratch),
    )(*args)


def group_size(members):
    return 4 if members % 4 == 0 else 2 if members % 2 == 0 else 1


def shape(dims, dtype):
    return jax.ShapeDtypeStruct(dims, dtype)


def first_kernel(n, size, group, *refs):
    own = refs[:n]
    near = refs[n : 2 * n]
    far = refs[2 * n : 3 * n]
    pert, tables, vert, inc, inc_half, acc = refs[3 * n :]
    rows = group * vert_rows(vert, group)
    lev = rows // group
    acc[...] = jnp.zeros_like(acc)
    t0, t1, t2 = tables[0], tables[3], tables[4]
    mix = vert[...]
    for ch in range(n):

        def step(g, _, ch=ch):
            at = pl.ds(g * group, group)
            spread = dot(own[ch][at].reshape(rows, CELLS), t0)
            spread += dot(near[ch][at].reshape(rows, CELLS), t1)
            spread += dot(far[ch][at].reshape(rows, CELLS), t2)
            local = dot(mix, spread.astype(BF16))
            for s in range(SLOTS):
                total = acc[s]
                for j in range(group):
                    weight = pert[ch * size + g * group + j, s].astype(F32)
                    total += weight * local[j * lev : (j + 1) * lev]
                acc[s] = total
            return 0

        lax.fori_loop(0, size // group, step, 0)
    inc[...] = acc[...]
    inc_half[...] = acc[...].astype(BF16)


def vert_rows(vert, group):
    return vert.shape[0] // group


def first_forward(own, near, far, pert, tables, vert, lev):
    n, size = len(own), own[0].shape[0]
    group = group_size(size)
    out = (shape((SLOTS, lev, CELLS), F32), shape((SLOTS, lev, CELLS), BF16))
    args = [*own, *near, *far, pert, tables, vert]
    return call(
        functools.partial(first_kernel, n, size, group), out, args, [pltpu.VMEM((SLOTS, lev, CELLS), F32)]
    )


def turn_kernel(n, size, group, sign, *refs):
    near = refs[:n]
    far = refs[n : 2 * n]
    adj_own, adj_other, base, pert, tables, vert, vert_t, vec, inc, inc_half, square, adj, acc = refs[2 * n :]
    rows = vert.shape[0]
    lev = rows // group
    adj[...] = adj_own[...] + adj_other[...].astype(F32)
    acc[...] = jnp.zeros_like(acc)
    square[...] = jnp.zeros_like(square)
    mix, mix_t = vert[...], vert_t[...]
    for ch in range(n):

        def step(g, _, ch=ch):
            sources = (
                lambda j, s: pert[ch * size + g * group + j, s],
                lambda j, s: near[ch][g * group + j, s],
                lambda j, s: far[ch][g * group + j, s],
            )
            back = None
            for t in range(3):
                projected = [
                    sources[t](j, 0).astype(F32) * adj[t, 0] + sources[t](j, 1).astype(F32) * adj[t, 1]
                    for j in range(group)
                ]
                projected = jnp.concatenate([p.astype(BF16) for p in projected], axis=0)
                lifted = dot(mix_t, projected).astype(BF16)
                part = dot(lifted, tables[t], ((1,), (1,)))
                back = part if back is None else back + part
            at = pl.ds(ch * size + g * group, group)
            new = base[at].reshape(rows, CELLS) + back
            if sign < 0:
                new = -new
            vec[at] = new.reshape(group, lev, CELLS)
            square[...] += jnp.sum((new * new).reshape(rows // 8, 8, CELLS), axis=0)
            half = new.astype(BF16)
            for t in range(3):
                spread = dot(half, tables[t]).astype(BF16)
                local = dot(mix, spread)
                for s in range(SLOTS):
                    total = acc[t, s]
                    for j in range(group):
                        total += sources[t](j, s).astype(F32) * local[j * lev : (j + 1) * lev]
                    acc[t, s] = total
            return 0

        lax.fori_loop(0, size // group, step, 0)
    inc[...] = acc[...]
    inc_half[...] = acc[...].astype(BF16)


def turn(adj_own, adj_other, base, pert, near, far, tables, vert, vert_t, sign):
    n, size = len(near), near[0].shape[0]
    lev = base.shape[1]
    group = group_size(size)
    field = (3, SLOTS, lev, CELLS)
    out = (shape(base.shape, F32), shape(field, F32), shape(field, BF16), shape((8, CELLS), F32))
    args = [*near, *far, adj_own, adj_other, base, pert, tables, vert, vert_t]
    return call(
        functools.partial(turn_kernel, n, size, group, sign),
        out,
        args,
        [pltpu.VMEM(field, F32), pltpu.VMEM(field, F32)],
    )


def three_pieces(row, rows):
    high = row.astype(BF16).astype(F32)
    mid = (row - high).astype(BF16).astype(F32)
    low = row - high - mid
    index = lax.broadcasted_iota(jnp.int32, (rows, row.shape[1]), 0)
    tile = jnp.where(index == 0, high, jnp.where(index == 1, mid, jnp.where(index == 2, low, 0.0)))
    return tile.astype(BF16)


def sample_kernel(regions, cap, kinds, inc, other, onehot, scal, out):
    for t in range(kinds):
        total = (inc[t] + other[t].astype(F32)).astype(BF16)
        cells = jnp.concatenate([total[s] for s in range(SLOTS)], axis=1)
        rows = dot(onehot[t], cells, ((1,), (1,))).astype(BF16)
        for h in range(regions):
            out[h, t * cap : (t + 1) * cap] = rows[h * cap : (h + 1) * cap]
    if out.shape[1] > kinds * cap:
        tile = three_pieces(scal[...], out.shape[1] - kinds * cap)
        for h in range(regions):
            out[h, kinds * cap :] = tile


def sample_plain(regions, cap, kinds, extra, inc, other, onehot, scal):
    parts = []
    for t in range(kinds):
        total = (inc[t] + other[t].astype(F32)).astype(BF16)
        cells = jnp.concatenate([total[s] for s in range(SLOTS)], axis=1)
        rows = dot(onehot[t], cells, ((1,), (1,))).astype(BF16)
        parts.append(rows.reshape(regions, cap, -1))
    if extra:
        tile = three_pieces(scal, extra)
        parts.append(jnp.broadcast_to(tile[None], (regions,) + tile.shape))
    return jnp.concatenate(parts, axis=1)


def sample(regions, cap, inc, other, onehot, scal=None):
    kinds, lev = inc.shape[0], inc.shape[2]
    extra = 0 if scal is None else 16
    if scal is None:
        scal = jnp.zeros((1, lev), F32)
    if cap % 16:
        return sample_plain(regions, cap, kinds, extra, inc, other, onehot, scal)
    return call(
        functools.partial(sample_kernel, regions, cap, kinds),
        shape((regions, kinds * cap + extra, lev), BF16),
        [inc, other, onehot, scal],
    )


def gathered(regions, cap, kinds, recv):
    parts = []
    for e in range(regions):
        total = recv[e, 0:cap].astype(F32)
        for t in range(1, kinds):
            source = side(e, t, regions)
            if source is not None:
                total = total + recv[source, t * cap : (t + 1) * cap].astype(F32)
        parts.append(total)
    return jnp.concatenate(parts, axis=0)


def placed_rows(pick, slots):
    high = slots.astype(BF16)
    low = (slots - high.astype(F32)).astype(BF16)
    return dot(pick, high) + dot(pick, low)


def weigh(tiles, rows):
    parts = [
        dot(tiles[i], rows[i * TILE : (i + 1) * TILE], precision=lax.Precision.HIGHEST)
        for i in range(tiles.shape[0])
    ]
    return jnp.concatenate(parts, axis=0)


def weigh_kernel(regions, cap, kinds, recv, pick, pick_t, tiles, innov, out, dep_out, wgt_out):
    dep = placed_rows(pick[...], gathered(regions, cap, kinds, recv)) - innov[...]
    wgt = weigh(tiles, dep)
    dep_out[...] = dep
    wgt_out[...] = wgt
    back = dot(pick_t[...], wgt.astype(BF16)).astype(BF16)
    for r in range(regions):
        for t in range(3):
            source = side(r, t, regions)
            if source is None:
                out[r, t * cap : (t + 1) * cap] = jnp.zeros((cap, back.shape[1]), BF16)
            else:
                out[r, t * cap : (t + 1) * cap] = back[source * cap : (source + 1) * cap]


def weigh_plain(regions, cap, kinds, recv, pick, pick_t, tiles, innov):
    dep = placed_rows(pick, gathered(regions, cap, kinds, recv)) - innov
    wgt = weigh(tiles, dep)
    back = dot(pick_t, wgt.astype(BF16)).astype(BF16).reshape(regions, cap, -1)
    return spread_regions(back, jnp.zeros((), BF16)), dep, wgt


def spread_regions(back, fill):
    regions = back.shape[0]
    tail = back.shape[1:]
    near = back.reshape((regions // 2, 2) + tail)[:, ::-1].reshape(back.shape)
    inner = back[1 : regions - 1].reshape((regions // 2 - 1, 2) + tail)[:, ::-1]
    blank = jnp.broadcast_to(fill, (1,) + tail)
    far = jnp.concatenate([blank, inner.reshape((regions - 2,) + tail), blank], axis=0)
    return jnp.concatenate([back, near, far], axis=1)


def weighed(regions, cap, recv, pick, pick_t, tiles, innov):
    lev = recv.shape[2]
    kinds = recv.shape[1] // cap
    obs = pick.shape[0]
    if cap % 16:
        return weigh_plain(regions, cap, kinds, recv, pick, pick_t, tiles, innov)
    out = (shape((regions, 3 * cap, lev), BF16), shape((obs, lev), F32), shape((obs, lev), F32))
    return call(
        functools.partial(weigh_kernel, regions, cap, kinds), out, [recv, pick, pick_t, tiles, innov]
    )


def scatter_kernel(regions, cap, recv, onehot_t, out, half):
    for t in range(3):
        rows = jnp.concatenate([recv[h, t * cap : (t + 1) * cap] for h in range(regions)], axis=0)
        field = dot(onehot_t[t], rows).T
        for s in range(SLOTS):
            piece = field[:, s * CELLS : (s + 1) * CELLS]
            out[t, s] = piece
            half[t, s] = piece.astype(BF16)


def scatter_plain(regions, cap, recv, onehot_t):
    lev = recv.shape[2]
    parts = []
    for t in range(3):
        rows = recv[:, t * cap : (t + 1) * cap].reshape(regions * cap, lev)
        field = dot(onehot_t[t], rows).T
        parts.append(jnp.stack([field[:, s * CELLS : (s + 1) * CELLS] for s in range(SLOTS)]))
    full = jnp.stack(parts)
    return full, full.astype(BF16)


def scattered(regions, cap, recv, onehot_t):
    lev = recv.shape[2]
    if cap % 16:
        return scatter_plain(regions, cap, recv, onehot_t)
    field = (3, SLOTS, lev, CELLS)
    return call(
        functools.partial(scatter_kernel, regions, cap),
        (shape(field, F32), shape(field, BF16)),
        [recv, onehot_t],
    )


def to_regions(values):
    return lax.all_to_all(values, "region", split_axis=0, concat_axis=0, tiled=True)


def other_members(own, half):
    if lax.axis_size("member") == 2:
        return own, lax.ppermute(half, "member", [(0, 1), (1, 0)])
    return lax.psum(half, "member").astype(F32), jnp.zeros_like(half)


def all_sum(values):
    regions = lax.axis_size("region")
    row = jnp.zeros((8, 128), F32).at[0, : values.shape[0]].set(values)
    total = jnp.sum(to_regions(jnp.broadcast_to(row, (regions, 8, 128))), axis=0)
    if lax.axis_size("member") == 2:
        total = total + lax.ppermute(total, "member", [(0, 1), (1, 0)])
    else:
        total = lax.psum(total, "member")
    return total[0, : values.shape[0]]


def member_sum(values):
    if lax.axis_size("member") == 2:
        return values + lax.ppermute(values, "member", [(0, 1), (1, 0)])
    return lax.psum(values, "member")


def local(
    perturbations,
    control,
    vertical_loc,
    block_kernels,
    loc_pattern,
    obs_region,
    obs_slot,
    obs_cell,
    innovations,
    obs_weight,
):
    regions = lax.axis_size("region")
    members = lax.axis_size("member")
    region = lax.axis_index("region")
    member = lax.axis_index("member")
    count, lev, _ = control.shape
    even = region % 2 == 0
    obs = obs_region.shape[0] // members
    cap = max(2, 2 * obs // regions)

    padded = jnp.pad(loc_pattern, ((1, 1), (0, 0)))
    before, here, after = (
        lax.dynamic_index_in_dim(padded, region + i, 0, keepdims=False) for i in range(3)
    )
    picks = jnp.stack(
        [
            here[1],
            jnp.where(even, after[0], before[2]),
            jnp.where(even, before[2], after[0]),
            jnp.where(even, here[2], here[0]),
            jnp.where(even, here[0], here[2]),
        ]
    )
    kinds = jnp.arange(block_kernels.shape[0], dtype=jnp.int32)
    tables = jnp.einsum(
        "bk,kij->bij", (picks[:, None] == kinds[None, :]).astype(BF16), block_kernels,
        preferred_element_type=F32,
    ).astype(BF16)

    chunks = HALO_CHUNKS if count % (4 * HALO_CHUNKS) == 0 else 1
    size = count // chunks
    group = group_size(size)
    eye = jnp.asarray(np.eye(group), BF16)
    vert = (eye[:, None, :, None] * vertical_loc[None, :, None, :]).reshape(group * lev, group * lev)
    vert_t = (eye[:, None, :, None] * vertical_loc.T[None, :, None, :]).reshape(group * lev, group * lev)

    start_half = control.astype(BF16)
    start_chunks = [start_half[i * size : (i + 1) * size] for i in range(chunks)]
    near_x, far_x = halo(start_chunks)
    near_p, far_p = halo([perturbations[i * size : (i + 1) * size] for i in range(chunks)])

    first = member * obs
    targets = lax.dynamic_slice_in_dim(obs_region[:, 0], first, obs, 0)
    codes = lax.dynamic_slice_in_dim(obs_slot * CELLS + obs_cell, first, obs, 0)
    innov = lax.dynamic_slice_in_dim(innovations, first, obs, 1).T
    tiles = lax.dynamic_slice_in_dim(obs_weight, member * (obs // TILE), obs // TILE, 0)
    named = targets[:, None] == jnp.arange(regions, dtype=jnp.int32)[None, :]
    lower = jnp.asarray(np.tril(np.ones((obs, obs)), -1), BF16)
    earlier = dot(lower, named.astype(BF16))
    rank = jnp.sum(jnp.where(named, earlier, 0.0), axis=1).astype(jnp.int32)
    position = targets * cap + rank
    slots = jnp.arange(regions * cap, dtype=jnp.int32)
    pick = (position[:, None] == slots[None, :]).astype(BF16)
    pick_t = (slots[:, None] == position[None, :]).astype(BF16)
    slot_codes = dot(pick_t, (codes + 1).astype(BF16)[:, None])[:, 0].astype(jnp.int32) - 1
    sent_codes = spread_regions(slot_codes.reshape(regions, cap), jnp.full((), -1, jnp.int32))
    got_codes = to_regions(sent_codes).reshape(regions, 3, cap).transpose(1, 0, 2).reshape(3, regions * cap)
    code_ids = jnp.arange(CODES, dtype=jnp.int32)
    onehot = (got_codes[:, :, None] == code_ids[None, None, :]).astype(BF16)
    onehot_t = (code_ids[None, :, None] == got_codes[:, None, :]).astype(BF16)

    no_innov = jnp.zeros_like(innov)

    inc, half = first_forward(start_chunks, near_x, far_x, perturbations, tables, vert, lev)
    inc, other = other_members(inc, half)
    recv = to_regions(sample(regions, cap, inc[None], other[None], onehot))
    back, _, _ = weighed(regions, cap, recv, pick, pick_t, tiles, innov)
    adj, adj_half = scattered(regions, cap, to_regions(back), onehot_t)
    adj, adj_other = other_members(adj, adj_half)
    resid, inc, half, square = turn(
        adj, adj_other, control, perturbations, near_p, far_p, tables, vert, vert_t, -1
    )

    inc, other = other_members(inc, half)
    recv = to_regions(sample(regions, cap, inc, other, onehot))
    back, dep, wgt = weighed(regions, cap, recv, pick, pick_t, tiles, no_innov)
    scal = member_sum(
        jnp.zeros((1, lev), F32).at[0, 0].set(jnp.sum(square)).at[0, 1].set(jnp.sum(dep * wgt))
    )
    adj, adj_half = scattered(regions, cap, to_regions(back), onehot_t)
    adj, adj_other = other_members(adj, adj_half)
    image, inc, half, _ = turn(
        adj, adj_other, resid, perturbations, near_p, far_p, tables, vert, vert_t, 1
    )

    inc, other = other_members(inc, half)
    recv = to_regions(sample(regions, cap, inc, other, onehot, scal))
    pieces = jnp.sum(recv[:, 3 * cap : 3 * cap + 3].astype(F32), axis=(0, 1))
    norm, seen = pieces[0], pieces[1]
    step = norm / (norm + seen)
    dep_image = placed_rows(pick, gathered(regions, cap, 3, recv))
    dep_next = dep - step * dep_image
    wgt_next = weigh(tiles, dep_next)
    resid_next = resid - step * image
    sums = all_sum(
        jnp.stack(
            [
                jnp.sum(resid_next * resid_next),
                jnp.sum(resid_next * resid),
                jnp.sum(dep_next * wgt_next),
                jnp.sum(dep_next * wgt),
            ]
        )
    )
    norm_next, mixed, seen_next, seen_mixed = sums[0], sums[1], sums[2], sums[3]
    ratio = norm_next / norm
    curved = norm_next + seen_next + 2.0 * ratio * (mixed + seen_mixed) + ratio * ratio * (norm + seen)
    step_next = norm_next / curved
    return control + step * resid + step_next * (resid_next + ratio * resid)


def solution(mesh):
    placed = (
        P("member", None, None, "region"),
        P("member", None, "region"),
        P(),
        P(),
        P(),
        P("region", None),
        P("region"),
        P("region"),
        P(None, "region"),
        P("region", None, None),
    )
    return jax.shard_map(
        local, mesh=mesh, in_specs=placed, out_specs=P("member", None, "region"), check_vma=False
    )
```

```python
import functools

import jax
import jax.numpy as jnp
import numpy as np
from jax import lax
from jax.experimental import pallas as pl
from jax.experimental.pallas import tpu as pltpu
from jax.sharding import PartitionSpec as P

SLOTS = 2
TILE = 128
CELLS = 128
ITERS = 2
CODES = SLOTS * CELLS
F32 = jnp.float32
BF16 = jnp.bfloat16
HALO_CHUNKS = 2


def near_of(r, regions):
    return r ^ 1


def far_of(r, regions):
    other = r - 1 if r % 2 == 0 else r + 1
    return other if 0 <= other < regions else None


def side(r, t, regions):
    return (r, near_of(r, regions), far_of(r, regions))[t]


def dot(a, b, dims=((1,), (0,)), precision=None):
    return lax.dot_general(a, b, (dims, ((), ())), precision=precision, preferred_element_type=F32)


def halo(chunks):
    regions = lax.axis_size("region")
    pairs = [(r, r ^ 1) for r in range(regions)]
    onward = [(r, r + 2 if r % 2 == 0 else r - 2) for r in range(regions)]
    onward = [(s, d) for s, d in onward if 0 <= d < regions]
    near = [lax.ppermute(c, "region", pairs) for c in chunks]
    far = [lax.ppermute(c, "region", onward) for c in near]
    return near, far


def call(kernel, out_shape, args, scratch=(), limit=16):
    return pl.pallas_call(
        kernel,
        out_shape=out_shape,
        in_specs=[pl.BlockSpec(memory_space=pltpu.VMEM)] * len(args),
        out_specs=jax.tree.map(lambda _: pl.BlockSpec(memory_space=pltpu.VMEM), out_shape),
        scratch_shapes=list(scratch),
        compiler_params=pltpu.CompilerParams(vmem_limit_bytes=limit << 20),
    )(*[pltpu.with_memory_space_constraint(a, pltpu.VMEM) for a in args])


def group_size(members):
    return 4 if members % 4 == 0 else 2 if members % 2 == 0 else 1


def shape(dims, dtype):
    return pltpu.VMEM(dims, dtype)


def first_kernel(n, size, group, *refs):
    own = refs[:n]
    near = refs[n : 2 * n]
    far = refs[2 * n : 3 * n]
    pert, stack, vert, inc, inc_half, acc = refs[3 * n :]
    rows = vert.shape[0]
    lev = rows // group
    acc[...] = jnp.zeros_like(acc)
    mix, tables = vert[...], stack[...]
    for ch in range(n):

        def step(g, _, ch=ch):
            at = pl.ds(g * group, group)
            values = jnp.concatenate(
                [part[ch][at].reshape(rows, CELLS) for part in (own, near, far)], axis=1
            )
            local = dot(mix, dot(values, tables).astype(BF16))
            for s in range(SLOTS):
                total = acc[s]
                for j in range(group):
                    weight = pert[ch * size + g * group + j, s].astype(F32)
                    total += weight * local[j * lev : (j + 1) * lev]
                acc[s] = total
            return 0

        lax.fori_loop(0, size // group, step, 0, unroll=size // group)
    inc[...] = acc[...]
    inc_half[...] = acc[...].astype(BF16)


def first_forward(own, near, far, pert, stack, vert, lev):
    n, size = len(own), own[0].shape[0]
    group = group_size(size)
    out = (shape((SLOTS, lev, CELLS), F32), shape((SLOTS, lev, CELLS), BF16))
    args = [*own, *near, *far, pert, stack, vert]
    return call(
        functools.partial(first_kernel, n, size, group), out, args, [pltpu.VMEM((SLOTS, lev, CELLS), F32)]
    )


def turn_kernel(n, size, group, sign, *refs):
    near = refs[:n]
    far = refs[n : 2 * n]
    adj_own, adj_other, base, pert, tables, vert, vert_t, vec, inc, inc_half, square, adj, acc = refs[2 * n :]
    rows = vert.shape[0]
    lev = rows // group
    adj[...] = adj_own[...] + adj_other[...].astype(F32)
    acc[...] = jnp.zeros_like(acc)
    square[...] = jnp.zeros_like(square)

    def source(t, ch, g, j, s):
        if t == 0:
            return pert[ch * size + g * group + j, s].astype(F32)
        return (near if t == 1 else far)[ch][g * group + j, s].astype(F32)

    def backward(ch, g):
        parts = []
        for t in range(3):
            parts.append(
                jnp.concatenate(
                    [
                        (source(t, ch, g, j, 0) * adj[t, 0] + source(t, ch, g, j, 1) * adj[t, 1]).astype(BF16)
                        for j in range(group)
                    ],
                    axis=0,
                )
            )
        moved = dot(jnp.concatenate(parts, axis=1), tables[...], ((1,), (1,))).astype(BF16)
        back = dot(vert_t[...], moved)
        at = pl.ds(ch * size + g * group, group)
        new = base[at].reshape(rows, CELLS) + back
        if sign < 0:
            new = -new
        vec[at] = new.reshape(group, lev, CELLS)
        square[...] += jnp.sum((new * new).reshape(rows // 8, 8, CELLS), axis=0)

    def forward(ch, g):
        at = pl.ds(ch * size + g * group, group)
        half = vec[at].reshape(rows, CELLS).astype(BF16)
        local = dot(dot(vert[...], half).astype(BF16), tables[...])
        for t in range(3):
            for s in range(SLOTS):
                total = acc[t, s]
                for j in range(group):
                    total += source(t, ch, g, j, s) * local[j * lev : (j + 1) * lev, t * CELLS : (t + 1) * CELLS]
                acc[t, s] = total

    steps = size // group
    for ch in range(n):
        backward(ch, 0)
        if ch:
            forward(ch - 1, steps - 1)

        def step(g, _, ch=ch):
            backward(ch, g)
            forward(ch, g - 1)
            return 0

        lax.fori_loop(1, steps, step, 0)
    forward(n - 1, steps - 1)
    inc[...] = acc[...]
    inc_half[...] = acc[...].astype(BF16)


def turn(adj_own, adj_other, base, pert, near, far, tables, vert, vert_t, sign):
    n, size = len(near), near[0].shape[0]
    lev = base.shape[1]
    group = group_size(size)
    field = (3, SLOTS, lev, CELLS)
    out = (shape(base.shape, F32), shape(field, F32), shape(field, BF16), shape((8, CELLS), F32))
    args = [*near, *far, adj_own, adj_other, base, pert, tables, vert, vert_t]
    return call(
        functools.partial(turn_kernel, n, size, group, sign),
        out,
        args,
        [pltpu.VMEM(field, F32), pltpu.VMEM(field, F32)],
    )


def three_pieces(row, rows):
    high = row.astype(BF16).astype(F32)
    mid = (row - high).astype(BF16).astype(F32)
    low = row - high - mid
    index = lax.broadcasted_iota(jnp.int32, (rows, row.shape[1]), 0)
    tile = jnp.where(index == 0, high, jnp.where(index == 1, mid, jnp.where(index == 2, low, 0.0)))
    return tile.astype(BF16)


def twice(cells):
    blank = jnp.zeros_like(cells)
    return jnp.concatenate(
        [jnp.concatenate([cells, blank], axis=1), jnp.concatenate([blank, cells], axis=1)], axis=0
    )


def scalar_row(values, width):
    lane = lax.broadcasted_iota(jnp.int32, (1, width), 1)
    row = jnp.zeros((1, width), F32)
    for i, value in enumerate(values):
        row = jnp.where(lane == i, value, row)
    return row


def sampled_rows(inc, other, onehot, t):
    total = (inc[t] + other[t].astype(F32)).astype(BF16)
    cells = jnp.concatenate([total[s] for s in range(SLOTS)], axis=1)
    return dot(onehot[t], twice(cells), ((1,), (1,))).astype(BF16)


def sample_kernel(regions, rows, kinds, inc, other, onehot, *refs):
    out = refs[-1]
    for t in range(kinds):
        found = sampled_rows(inc, other, onehot, t)
        for h in range(regions):
            out[h, t * rows : (t + 1) * rows] = found[h * rows : (h + 1) * rows]
    if len(refs) > 1:
        tile = three_pieces(scalar_row([jnp.sum(ref[...]) for ref in refs[:-1]], out.shape[2]), 16)
        for h in range(regions):
            out[h, kinds * rows :] = tile


def sample(regions, rows, inc, other, onehot, scal=()):
    kinds, lev = inc.shape[0], inc.shape[2]
    extra = 16 if scal else 0
    if rows % 16:
        parts = [sampled_rows(inc, other, onehot, t).reshape(regions, rows, 2 * lev) for t in range(kinds)]
        if scal:
            tile = three_pieces(scalar_row([jnp.sum(v) for v in scal], 2 * lev), 16)
            parts.append(jnp.broadcast_to(tile[None], (regions,) + tile.shape))
        return jnp.concatenate(parts, axis=1)
    return call(
        functools.partial(sample_kernel, regions, rows, kinds),
        shape((regions, kinds * rows + extra, 2 * lev), BF16),
        [inc, other, onehot, *scal],
    )


def gathered(regions, rows, kinds, recv):
    parts = []
    for e in range(regions):
        total = recv[e, 0:rows].astype(F32)
        for t in range(1, kinds):
            source = side(e, t, regions)
            if source is not None:
                total = total + recv[source, t * rows : (t + 1) * rows].astype(F32)
        parts.append(total)
    return jnp.concatenate(parts, axis=0)


def swap_lanes(values):
    half = values.shape[1] // 2
    return jnp.concatenate([values[:, half:], values[:, :half]], axis=1)


def both_parts(values):
    high = values.astype(BF16)
    low = (values - high.astype(F32)).astype(BF16)
    return high, low


def departures(regions, rows, kinds, recv, pick):
    slots = gathered(regions, rows, kinds, recv)
    high = slots.astype(BF16).astype(F32)
    low = swap_lanes(slots - high)
    first = lax.broadcasted_iota(jnp.int32, slots.shape, 1) < slots.shape[1] // 2
    stacked = jnp.concatenate([jnp.where(first, high, low), jnp.where(first, low, high)], axis=0)
    found = dot(pick, stacked.astype(BF16))
    return found + swap_lanes(found)


def weigh(tiles, both):
    high = both.astype(BF16).astype(F32)
    first = lax.broadcasted_iota(jnp.int32, both.shape, 1) < both.shape[1] // 2
    split = jnp.where(first, high, both - high).astype(BF16)
    parts = []
    for i in range(tiles.shape[0]):
        own = split[i * TILE : (i + 1) * TILE]
        parts.append(dot(tiles[i], jnp.concatenate([own, own], axis=0)))
    out = jnp.concatenate(parts, axis=0)
    return out + swap_lanes(out)


def halves_apart(both):
    first = lax.broadcasted_iota(jnp.int32, both.shape, 1) < both.shape[1] // 2
    return jnp.concatenate([jnp.where(first, both, 0.0), jnp.where(first, 0.0, both)], axis=0).astype(BF16)


def column_sums(values):
    return jnp.sum(values.reshape(values.shape[0] // 8, 8, values.shape[1]), axis=0)


def weigh_kernel(regions, rows, kinds, recv, pick, pick_t, tiles, innov, out, dep_out, wgt_out, seen):
    dep = departures(regions, rows, kinds, recv, pick[...])
    if innov is not None:
        dep = dep - innov[...]
    wgt = weigh(tiles, dep)
    dep_out[...] = dep
    wgt_out[...] = wgt
    seen[...] = column_sums(0.5 * dep * wgt)
    back = dot(pick_t[...], halves_apart(wgt)).astype(BF16)
    for r in range(regions):
        for t in range(3):
            source = side(r, t, regions)
            if source is None:
                out[r, t * rows : (t + 1) * rows] = jnp.zeros((rows, back.shape[1]), BF16)
            else:
                out[r, t * rows : (t + 1) * rows] = back[source * rows : (source + 1) * rows]


def weigh_later_kernel(regions, rows, kinds, recv, pick, pick_t, tiles, out, dep_out, wgt_out, seen):
    weigh_kernel(regions, rows, kinds, recv, pick, pick_t, tiles, None, out, dep_out, wgt_out, seen)


def spread_regions(back, fill):
    regions = back.shape[0]
    tail = back.shape[1:]
    near = back.reshape((regions // 2, 2) + tail)[:, ::-1].reshape(back.shape)
    inner = back[1 : regions - 1].reshape((regions // 2 - 1, 2) + tail)[:, ::-1]
    blank = jnp.broadcast_to(fill, (1,) + tail)
    far = jnp.concatenate([blank, inner.reshape((regions - 2,) + tail), blank], axis=0)
    return jnp.concatenate([back, near, far], axis=1)


def weighed(regions, rows, recv, pick, pick_t, tiles, innov=None):
    lanes = recv.shape[2]
    kinds = recv.shape[1] // rows
    obs = pick.shape[0]
    if rows % 16:
        dep = departures(regions, rows, kinds, recv, pick)
        dep = dep if innov is None else dep - innov
        wgt = weigh(tiles, dep)
        back = dot(pick_t, halves_apart(wgt)).astype(BF16).reshape(regions, rows, lanes)
        return spread_regions(back, jnp.zeros((), BF16)), dep, wgt, column_sums(0.5 * dep * wgt)
    out = (
        shape((regions, 3 * rows, lanes), BF16),
        shape((obs, lanes), F32),
        shape((obs, lanes), F32),
        shape((8, lanes), F32),
    )
    args = [recv, pick, pick_t, tiles] + ([] if innov is None else [innov])
    kernel = weigh_later_kernel if innov is None else weigh_kernel
    return call(functools.partial(kernel, regions, rows, kinds), out, args)


def scattered_field(rows_t, onehot_t, lev):
    count = rows_t.shape[0]
    low = dot(onehot_t[:, :count], rows_t).T
    high = dot(onehot_t[:, count:], rows_t).T
    return low[:lev] + high[lev:]


def scatter_kernel(regions, rows, recv, onehot_t, out, half):
    lev = out.shape[2]
    for t in range(3):
        values = jnp.concatenate([recv[h, t * rows : (t + 1) * rows] for h in range(regions)], axis=0)
        field = scattered_field(values, onehot_t[t], lev)
        for s in range(SLOTS):
            piece = field[:, s * CELLS : (s + 1) * CELLS]
            out[t, s] = piece
            half[t, s] = piece.astype(BF16)


def scattered(regions, rows, recv, onehot_t):
    lanes = recv.shape[2]
    lev = lanes // 2
    if rows % 16:
        parts = []
        for t in range(3):
            values = recv[:, t * rows : (t + 1) * rows].reshape(regions * rows, lanes)
            field = scattered_field(values, onehot_t[t], lev)
            parts.append(jnp.stack([field[:, s * CELLS : (s + 1) * CELLS] for s in range(SLOTS)]))
        full = jnp.stack(parts)
        return full, full.astype(BF16)
    field = (3, SLOTS, lev, CELLS)
    return call(
        functools.partial(scatter_kernel, regions, rows),
        (shape(field, F32), shape(field, BF16)),
        [recv, onehot_t],
    )


def last_sums(regions, rows, recv, pick, tiles, dep, wgt, pieces, norms):
    total = jnp.sum(jnp.sum(pieces.astype(F32), axis=0), axis=0, keepdims=True)
    lane = lax.broadcasted_iota(jnp.int32, total.shape, 1)
    norm = jnp.sum(jnp.where(lane == 0, total, 0.0))
    seen = jnp.sum(jnp.where(lane == 1, total, 0.0))
    step = norm / (norm + seen)
    dep_image = departures(regions, rows, 3, recv, pick)
    dep_next = dep - step * dep_image
    wgt_next = weigh(tiles, dep_next)
    squares, mixed = norms(step)
    values = [
        squares,
        mixed,
        0.5 * jnp.sum(dep_next * wgt_next),
        0.5 * jnp.sum(dep_next * wgt),
    ]
    return scalar_row(values, 128), scalar_row([norm, seen, step], 128)


def last_kernel(regions, rows, group, recv, pick, tiles, dep, wgt, resid, image, out, known):
    count, lev, cells = resid.shape

    def norms(step):
        def add(g, carry):
            at = pl.ds(g * group, group)
            now = resid[at].reshape(group * lev, cells)
            later = now - step * image[at].reshape(group * lev, cells)
            return carry[0] + column_sums(later * later), carry[1] + column_sums(later * now)

        zero = jnp.zeros((8, cells), F32)
        squares, mixed = lax.fori_loop(0, count // group, add, (zero, zero))
        return jnp.sum(squares), jnp.sum(mixed)

    pieces = recv[:, 3 * rows : 3 * rows + 3]
    sums, facts = last_sums(regions, rows, recv, pick[...], tiles, dep[...], wgt[...], pieces, norms)
    wide = jnp.broadcast_to(sums, (8, 128))
    for r in range(regions):
        out[r] = wide
    known[...] = jnp.broadcast_to(facts, (8, 128))


def last(regions, rows, recv, pick, tiles, dep, wgt, resid, image):
    if rows % 16:

        def norms(step):
            later = resid - step * image
            return jnp.sum(later * later), jnp.sum(later * resid)

        sums, facts = last_sums(
            regions, rows, recv, pick, tiles, dep, wgt, recv[:, 3 * rows : 3 * rows + 3], norms
        )
        return jnp.broadcast_to(sums[None], (regions, 8, 128)), jnp.broadcast_to(facts, (8, 128))
    group = group_size(resid.shape[0])
    return call(
        functools.partial(last_kernel, regions, rows, group),
        (shape((regions, 8, 128), F32), shape((8, 128), F32)),
        [recv, pick, tiles, dep, wgt, resid, image],
    )


def to_regions(values):
    return lax.all_to_all(values, "region", split_axis=0, concat_axis=0, tiled=True)


def other_members(own, half):
    if lax.axis_size("member") == 2:
        return own, lax.ppermute(half, "member", [(0, 1), (1, 0)])
    return lax.psum(half, "member").astype(F32), jnp.zeros_like(half)


def member_sum(values):
    if lax.axis_size("member") == 2:
        return values + lax.ppermute(values, "member", [(0, 1), (1, 0)])
    return lax.psum(values, "member")


def local(
    perturbations,
    control,
    vertical_loc,
    block_kernels,
    loc_pattern,
    obs_region,
    obs_slot,
    obs_cell,
    innovations,
    obs_weight,
):
    regions = lax.axis_size("region")
    members = lax.axis_size("member")
    region = lax.axis_index("region")
    member = lax.axis_index("member")
    count, lev, _ = control.shape
    even = region % 2 == 0
    obs = obs_region.shape[0] // members
    cap = max(2, 2 * obs // regions)

    padded = jnp.pad(loc_pattern, ((1, 1), (0, 0)))
    before, here, after = (
        lax.dynamic_index_in_dim(padded, region + i, 0, keepdims=False) for i in range(3)
    )
    picks = jnp.stack(
        [
            here[1],
            jnp.where(even, after[0], before[2]),
            jnp.where(even, before[2], after[0]),
            jnp.where(even, here[2], here[0]),
            jnp.where(even, here[0], here[2]),
        ]
    )
    kinds = jnp.arange(block_kernels.shape[0], dtype=jnp.int32)
    picked = jnp.einsum(
        "bk,kij->bij", (picks[:, None] == kinds[None, :]).astype(BF16), block_kernels,
        preferred_element_type=F32,
    ).astype(BF16)
    tables = jnp.concatenate([picked[0], picked[1], picked[2]], axis=1)
    stack = jnp.concatenate([picked[0], picked[3], picked[4]], axis=0)

    chunks = HALO_CHUNKS if count % (4 * HALO_CHUNKS) == 0 else 1
    size = count // chunks
    group = group_size(size)
    eye = jnp.asarray(np.eye(group), BF16)
    vert = (eye[:, None, :, None] * vertical_loc[None, :, None, :]).reshape(group * lev, group * lev)
    vert_t = (eye[:, None, :, None] * vertical_loc.T[None, :, None, :]).reshape(group * lev, group * lev)

    start_half = control.astype(BF16)
    start_chunks = [start_half[i * size : (i + 1) * size] for i in range(chunks)]
    near_x, far_x = halo(start_chunks)
    near_p, far_p = halo([perturbations[i * size : (i + 1) * size] for i in range(chunks)])

    first = member * obs
    targets = lax.dynamic_slice_in_dim(obs_region[:, 0], first, obs, 0)
    codes = lax.dynamic_slice_in_dim(obs_slot * CELLS + obs_cell, first, obs, 0)
    innov = lax.dynamic_slice_in_dim(innovations, first, obs, 1).T
    innov = jnp.concatenate([innov, innov], axis=1)
    tiles = lax.dynamic_slice_in_dim(obs_weight, member * (obs // TILE), obs // TILE, 0)
    tiles_high = tiles.astype(BF16)
    tiles = jnp.concatenate([tiles_high, (tiles - tiles_high.astype(F32)).astype(BF16)], axis=2)
    named = targets[:, None] == jnp.arange(regions, dtype=jnp.int32)[None, :]
    lower = lax.broadcasted_iota(jnp.int32, (obs, obs), 0) > lax.broadcasted_iota(jnp.int32, (obs, obs), 1)
    earlier = dot(lower.astype(BF16), named.astype(BF16))
    rank = jnp.sum(jnp.where(named, earlier, 0.0), axis=1).astype(jnp.int32)
    rows = cap // 2
    slots_of_half = regions * rows
    position = (rank // rows) * slots_of_half + targets * rows + rank % rows
    slots = jnp.arange(2 * slots_of_half, dtype=jnp.int32)
    pick = (position[:, None] == slots[None, :]).astype(BF16)
    half_slots = jnp.arange(slots_of_half, dtype=jnp.int32)
    pick_t = jnp.concatenate(
        [
            (half_slots[:, None] == position[None, :]).astype(BF16),
            (half_slots[:, None] + slots_of_half == position[None, :]).astype(BF16),
        ],
        axis=1,
    )
    slot_codes = dot((slots[:, None] == position[None, :]).astype(BF16), (codes + 1).astype(BF16)[:, None])
    slot_codes = slot_codes[:, 0].astype(jnp.int32) - 1
    slot_codes = slot_codes.reshape(2, regions, rows).transpose(1, 0, 2)
    sent_codes = spread_regions(slot_codes, jnp.full((), -1, jnp.int32))
    sent_codes, near_x = lax.optimization_barrier((sent_codes, near_x))
    got_codes = to_regions(sent_codes.reshape(regions, 6 * rows)).reshape(regions, 3, 2, rows)
    got_codes = got_codes.transpose(1, 2, 0, 3).reshape(3, 2, slots_of_half)
    code_ids = jnp.arange(CODES, dtype=jnp.int32)
    onehot = jnp.concatenate(
        [(got_codes[:, i, :, None] == code_ids[None, None, :]).astype(BF16) for i in range(2)], axis=2
    )
    onehot_t = jnp.concatenate(
        [(code_ids[None, :, None] == got_codes[:, i, None, :]).astype(BF16) for i in range(2)], axis=2
    )

    inc, half = first_forward(start_chunks, near_x, far_x, perturbations, stack, vert, lev)
    inc, other = other_members(inc, half)
    recv = to_regions(sample(regions, rows, inc[None], other[None], onehot))
    back, _, _, _ = weighed(regions, rows, recv, pick, pick_t, tiles, innov)
    adj, adj_half = scattered(regions, rows, to_regions(back), onehot_t)
    adj, adj_other = other_members(adj, adj_half)
    resid, inc, half, square = turn(
        adj, adj_other, control, perturbations, near_p, far_p, tables, vert, vert_t, -1
    )

    inc, other = other_members(inc, half)
    recv = to_regions(sample(regions, rows, inc, other, onehot))
    back, dep, wgt, seen = weighed(regions, rows, recv, pick, pick_t, tiles)
    adj, adj_half = scattered(regions, rows, to_regions(back), onehot_t)
    adj, adj_other = other_members(adj, adj_half)
    square, seen = member_sum(square), member_sum(seen)
    image, inc, half, _ = turn(
        adj, adj_other, resid, perturbations, near_p, far_p, tables, vert, vert_t, 1
    )

    inc, other = other_members(inc, half)
    recv = to_regions(sample(regions, rows, inc, other, onehot, (square, seen)))
    sums, facts = last(regions, rows, recv, pick, tiles, dep, wgt, resid, image)
    sums = member_sum(jnp.sum(to_regions(sums), axis=0))[0]
    norm, seen, step = facts[0, 0], facts[0, 1], facts[0, 2]
    norm_next, mixed, seen_next, seen_mixed = sums[0], sums[1], sums[2], sums[3]
    ratio = norm_next / norm
    curved = norm_next + seen_next + 2.0 * ratio * (mixed + seen_mixed) + ratio * ratio * (norm + seen)
    step_next = norm_next / curved
    return control + (step + step_next * (1.0 + ratio)) * resid - (step_next * step) * image


def solution(mesh):
    placed = (
        P("member", None, None, "region"),
        P("member", None, "region"),
        P(),
        P(),
        P(),
        P("region", None),
        P("region"),
        P("region"),
        P(None, "region"),
        P("region", None, None),
    )
    return jax.shard_map(
        local, mesh=mesh, in_specs=placed, out_specs=P("member", None, "region"), check_vma=False
    )
```

```python
import functools

import jax
import jax.numpy as jnp
from jax import lax
from jax.experimental import pallas as pl
from jax.experimental.pallas import tpu as pltpu
from jax.sharding import PartitionSpec as P


SLOTS = 2
TILE = 128
CELLS = 128
CODES = SLOTS * CELLS
F32 = jnp.float32
BF16 = jnp.bfloat16
HALO_CHUNKS = 5


def near_of(r):
    return r ^ 1


def far_of(r, regions):
    other = r - 1 if r % 2 == 0 else r + 1
    return other if 0 <= other < regions else None


def side(r, t, regions):
    return (r, near_of(r), far_of(r, regions))[t]


def dot(a, b, dims=((1,), (0,)), precision=None):
    return lax.dot_general(a, b, (dims, ((), ())), precision=precision, preferred_element_type=F32)


def halo(chunks):
    regions = lax.axis_size("region")
    pairs = [(r, r ^ 1) for r in range(regions)]
    onward = [(r, r + 2 if r % 2 == 0 else r - 2) for r in range(regions)]
    onward = [(s, d) for s, d in onward if 0 <= d < regions]
    near = [lax.ppermute(c, "region", pairs) for c in chunks]
    far = [lax.ppermute(c, "region", onward) for c in near]
    return near, far


def call(kernel, out_shape, args, scratch=(), limit=16, scalars=()):
    vmem = pl.BlockSpec(memory_space=pltpu.VMEM)
    return pl.pallas_call(
        kernel,
        out_shape=out_shape,
        in_specs=[pl.BlockSpec(memory_space=pltpu.SMEM)] * len(scalars) + [vmem] * len(args),
        out_specs=jax.tree.map(lambda _: vmem, out_shape),
        scratch_shapes=list(scratch),
        compiler_params=pltpu.CompilerParams(vmem_limit_bytes=limit << 20),
    )(*scalars, *[pltpu.with_memory_space_constraint(a, pltpu.VMEM) for a in args])


def group_size(members):
    return 4 if members % 4 == 0 else 2 if members % 2 == 0 else 1


def shape(dims, dtype):
    return pltpu.VMEM(dims, dtype)


def block_diagonal(matrix, copies, transposed):
    size = matrix.shape[0]
    total = copies * size
    row = lax.broadcasted_iota(jnp.int32, (total, size), 0)
    place = (row % size == lax.broadcasted_iota(jnp.int32, (total, size), 1)).astype(BF16)
    tall = dot(place, matrix, ((1,), (1 if transposed else 0,))).astype(BF16)
    wide = dot(tall, place, ((1,), (1,)))
    same = (
        lax.broadcasted_iota(jnp.int32, (total, total), 0) // size
        == lax.broadcasted_iota(jnp.int32, (total, total), 1) // size
    )
    return jnp.where(same, wide, 0.0).astype(BF16)


def own_kernel(group, pattern, start, pert, kernels, vloc, inc, lifted, tables, vert, vert_t, acc):
    count, lev, _ = start.shape
    rows = group * lev
    acc[...] = jnp.zeros_like(acc)
    vert[...] = block_diagonal(vloc[...], group, False)
    vert_t[...] = block_diagonal(vloc[...], group, True)
    region = lax.axis_index("region")
    even = region % 2 == 0
    up = pattern[jnp.minimum(region + 1, pattern.shape[0] - 1), 0]
    down = pattern[jnp.maximum(region - 1, 0), 2]
    picks = (pattern[region, 1], jnp.where(even, up, down), jnp.where(even, down, up))
    for t in range(3):
        tables[:, t * CELLS : (t + 1) * CELLS] = kernels[picks[t]]

    def step(g, _):
        at = pl.ds(g * group, group)
        mixed = dot(vert[...], start[at].reshape(rows, CELLS).astype(BF16)).astype(BF16)
        lifted[at] = mixed.reshape(group, lev, CELLS)
        local = dot(mixed, tables[:, :CELLS])
        for s in range(SLOTS):
            total = acc[s]
            for j in range(group):
                total += pert[g * group + j, s].astype(F32) * local[j * lev : (j + 1) * lev]
            acc[s] = total
        return 0

    lax.fori_loop(0, count // group, step, 0, unroll=2)
    inc[...] = acc[...]


def own_forward(pattern, start, pert, kernels, vloc, group):
    _, lev, _ = start.shape
    field = (SLOTS, lev, CELLS)
    square = shape((group * lev, group * lev), BF16)
    out = (shape(field, F32), shape(start.shape, BF16), shape((CELLS, 3 * CELLS), BF16), square, square)
    return call(
        functools.partial(own_kernel, group),
        out,
        [start, pert, kernels, vloc],
        [pltpu.VMEM(field, F32)],
        scalars=[pattern],
    )


def part_sum(n, group, t, chunks, lifted, tables, acc, full):
    lev = lifted.shape[1]
    rows = group * lev
    acc[...] = jnp.zeros_like(acc)
    first = 0
    for ch in range(n):
        size = chunks[ch].shape[0]

        def step(g, _, ch=ch, first=first):
            at = pl.ds(first + g * group, group)
            local = dot(lifted[at].reshape(rows, CELLS), tables[:, t * CELLS : (t + 1) * CELLS])
            values = chunks[ch][pl.ds(g * group, group)]
            full[at] = values
            for s in range(SLOTS):
                total = acc[s]
                for j in range(group):
                    total += values[j, s].astype(F32) * local[j * lev : (j + 1) * lev]
                acc[s] = total
            return 0

        lax.fori_loop(0, size // group, step, 0, unroll=size // group)
        first += size


def near_kernel(n, group, *refs):
    chunks = refs[:n]
    lifted, tables, inc, full, acc = refs[n:]
    part_sum(n, group, 1, chunks, lifted, tables, acc, full)
    inc[...] = acc[...]


def joined(chunks):
    return shape((sum(c.shape[0] for c in chunks),) + chunks[0].shape[1:], chunks[0].dtype)


def near_forward(chunks, lifted, tables, group):
    field = (SLOTS, lifted.shape[1], CELLS)
    return call(
        functools.partial(near_kernel, len(chunks), group),
        (shape(field, F32), joined(chunks)),
        [*chunks, lifted, tables],
        [pltpu.VMEM(field, F32)],
    )


def far_kernel(n, group, *refs):
    chunks = refs[:n]
    own, near, lifted, tables, inc, half, full, acc = refs[n:]
    part_sum(n, group, 2, chunks, lifted, tables, acc, full)
    for t, part in enumerate((own, near, acc)):
        inc[t] = part[...]
        half[t] = part[...].astype(BF16)


def far_forward(chunks, own, near, lifted, tables, group):
    field = (SLOTS, lifted.shape[1], CELLS)
    return call(
        functools.partial(far_kernel, len(chunks), group),
        (shape((3,) + field, F32), shape((3,) + field, BF16), joined(chunks)),
        [*chunks, own, near, lifted, tables],
        [pltpu.VMEM(field, F32)],
    )


def columns(row, width):
    return jnp.broadcast_to(row.astype(F32), (width, row.shape[1])).T.astype(jnp.int32)


def lane_choice(column, start, width):
    lanes = lax.broadcasted_iota(jnp.int32, column.shape, 1)
    blocks = [jnp.where(column == lanes + (start + b), 1.0, 0.0).astype(BF16) for b in range(0, width, column.shape[1])]
    return blocks[0] if len(blocks) == 1 else jnp.concatenate(blocks, axis=1)


def row_choice(row, start, count):
    index = lax.broadcasted_iota(jnp.int32, (count, row.shape[1]), 0) + start
    return jnp.where(index == row, 1.0, 0.0).astype(BF16)


def code_rows(recv, rows):
    return [
        jnp.concatenate([recv[h, k : k + 1, :rows] for h in range(recv.shape[0])], axis=1) for k in range(6)
    ]


def selections(position, codes, weight, innov):
    half = codes[0].shape[1]
    column = columns(position, 128)
    pick = lane_choice(column, 0, 2 * half)
    pick_t = jnp.concatenate([row_choice(position, i * half, half) for i in range(2)], axis=1)
    onehot, onehot_t = [], []
    for t in range(3):
        pair = codes[2 * t : 2 * t + 2]
        onehot.append(jnp.concatenate([lane_choice(columns(row, 128), 0, CODES) for row in pair], axis=1))
        onehot_t.append(jnp.concatenate([row_choice(row, 0, CODES) for row in pair], axis=1))
    high = weight.astype(BF16)
    tiles = jnp.concatenate([high, (weight - high.astype(F32)).astype(BF16)], axis=2)
    turned = innov.T
    return pick, pick_t, onehot, onehot_t, tiles, jnp.concatenate([turned, turned], axis=1)


def selections_kernel(rows, position, codes, weight, innov, pick, pick_t, onehot, onehot_t, tiles, turned):
    obs = position.shape[1]
    member = lax.axis_index("member")
    kept = weight[pl.ds(member * (obs // TILE), obs // TILE)]
    seen = innov[:, pl.ds(pl.multiple_of(member * obs, obs), obs)]
    made = selections(position[0:1], code_rows(codes, rows), kept, seen)
    pick[...], pick_t[...] = made[0], made[1]
    for t in range(3):
        onehot[t], onehot_t[t] = made[2][t], made[3][t]
    tiles[...], turned[...] = made[4], made[5]


def select_all(rows, position, codes, weight, innov):
    obs = position.shape[1]
    half = codes.shape[0] * rows
    if rows % 16:
        member = lax.axis_index("member")
        kept = lax.dynamic_slice_in_dim(weight, member * (obs // TILE), obs // TILE, 0)
        seen = lax.dynamic_slice_in_dim(innov, member * obs, obs, 1)
        pick, pick_t, onehot, onehot_t, tiles, turned = selections(
            position[0:1], code_rows(codes, rows), kept, seen
        )
        return pick, pick_t, jnp.stack(onehot), jnp.stack(onehot_t), tiles, turned
    lev = innov.shape[0]
    out = (
        shape((obs, 2 * half), BF16),
        shape((half, 2 * obs), BF16),
        shape((3, half, 2 * CODES), BF16),
        shape((3, CODES, 2 * half), BF16),
        shape((obs // TILE, TILE, 2 * TILE), BF16),
        shape((obs, 2 * lev), F32),
    )
    return call(functools.partial(selections_kernel, rows), out, [position, codes, weight, innov])


def turn_kernel(group, sign, *refs):
    near, far, adj_own, adj_other, base, pert, tables, vert, vert_t, vec, inc, inc_half, square = refs[:13]
    adj, acc, moved, mixed = refs[13:]
    rows = vert.shape[0]
    lev = rows // group
    adj[...] = adj_own[...] + adj_other[...].astype(F32)
    acc[...] = jnp.zeros_like(acc)
    square[...] = jnp.zeros_like(square)
    sources = (pert, near, far)

    def project(g):
        parts = []
        for t in range(3):
            values = sources[t][pl.ds(g * group, group)].astype(F32)
            parts.append(
                jnp.concatenate(
                    [(values[j, 0] * adj[t, 0] + values[j, 1] * adj[t, 1]).astype(BF16) for j in range(group)],
                    axis=0,
                )
            )
        moved[g] = dot(jnp.concatenate(parts, axis=1), tables[...], ((1,), (1,))).astype(BF16)

    def lift(g):
        at = pl.ds(g * group, group)
        new = base[at].reshape(rows, CELLS) + dot(vert_t[...], moved[g])
        if sign < 0:
            new = -new
        vec[at] = new.reshape(group, lev, CELLS)
        square[...] += jnp.sum((new * new).reshape(rows // 8, 8, CELLS), axis=0)

    def mix(g):
        half = vec[pl.ds(g * group, group)].reshape(rows, CELLS).astype(BF16)
        mixed[g] = dot(vert[...], half).astype(BF16)

    def gather(g):
        local = dot(mixed[g], tables[...])
        for t in range(3):
            values = sources[t][pl.ds(g * group, group)]
            for s in range(SLOTS):
                total = acc[t, s]
                for j in range(group):
                    part = local[j * lev : (j + 1) * lev, t * CELLS : (t + 1) * CELLS]
                    total += values[j, s].astype(F32) * part
                acc[t, s] = total

    stages = (gather, mix, lift, project)
    steps = base.shape[0] // group
    depth = len(stages)
    for i in range(min(depth - 1, steps)):
        for k, stage in enumerate(stages):
            if 0 <= i - (depth - 1 - k):
                stage(i - (depth - 1 - k))

    def step(g, _):
        for k, stage in enumerate(stages):
            stage(g - (depth - 1 - k))
        return 0

    lax.fori_loop(depth - 1, steps, step, 0)
    for i in range(max(steps, depth - 1), steps + depth - 1):
        for k, stage in enumerate(stages):
            if 0 <= i - (depth - 1 - k) < steps:
                stage(i - (depth - 1 - k))
    inc[...] = acc[...]
    inc_half[...] = acc[...].astype(BF16)


def turn(adj_own, adj_other, base, pert, near, far, tables, vert, vert_t, sign):
    count, lev, _ = base.shape
    group = vert.shape[0] // lev
    field = (3, SLOTS, lev, CELLS)
    out = (shape(base.shape, F32), shape(field, F32), shape(field, BF16), shape((8, CELLS), F32))
    half = pltpu.VMEM((count // group, group * lev, CELLS), BF16)
    return call(
        functools.partial(turn_kernel, group, sign),
        out,
        [near, far, adj_own, adj_other, base, pert, tables, vert, vert_t],
        [pltpu.VMEM(field, F32), pltpu.VMEM(field, F32), half, half],
    )


def three_pieces(row, rows):
    high = row.astype(BF16).astype(F32)
    mid = (row - high).astype(BF16).astype(F32)
    low = row - high - mid
    index = lax.broadcasted_iota(jnp.int32, (rows, row.shape[1]), 0)
    tile = jnp.where(index == 0, high, jnp.where(index == 1, mid, jnp.where(index == 2, low, 0.0)))
    return tile.astype(BF16)


def twice(cells):
    blank = jnp.zeros_like(cells)
    return jnp.concatenate(
        [jnp.concatenate([cells, blank], axis=1), jnp.concatenate([blank, cells], axis=1)], axis=0
    )


def scalar_row(values, width):
    lane = lax.broadcasted_iota(jnp.int32, (1, width), 1)
    row = jnp.zeros((1, width), F32)
    for i, value in enumerate(values):
        row = jnp.where(lane == i, value, row)
    return row


def sampled_rows(inc, other, onehot, t):
    total = (inc[t] + other[t].astype(F32)).astype(BF16)
    cells = jnp.concatenate([total[s] for s in range(SLOTS)], axis=1)
    return dot(onehot[t], twice(cells), ((1,), (1,))).astype(BF16)


def sample_kernel(regions, rows, kinds, inc, other, onehot, *refs):
    out = refs[-1]
    for t in range(kinds):
        found = sampled_rows(inc, other, onehot, t)
        for h in range(regions):
            out[h, t * rows : (t + 1) * rows] = found[h * rows : (h + 1) * rows]
    if len(refs) > 1:
        tile = three_pieces(scalar_row([jnp.sum(ref[...]) for ref in refs[:-1]], out.shape[2]), 8)
        for h in range(regions):
            out[h, kinds * rows :] = tile


def sample(regions, rows, inc, other, onehot, scal=()):
    kinds, lev = inc.shape[0], inc.shape[2]
    extra = 8 if scal else 0
    if rows % 16:
        parts = [sampled_rows(inc, other, onehot, t).reshape(regions, rows, 2 * lev) for t in range(kinds)]
        if scal:
            tile = three_pieces(scalar_row([jnp.sum(v) for v in scal], 2 * lev), 8)
            parts.append(jnp.broadcast_to(tile[None], (regions,) + tile.shape))
        return jnp.concatenate(parts, axis=1)
    return call(
        functools.partial(sample_kernel, regions, rows, kinds),
        shape((regions, kinds * rows + extra, 2 * lev), BF16),
        [inc, other, onehot, *scal],
    )


def gathered(regions, rows, kinds, recv):
    parts = []
    for e in range(regions):
        total = recv[e, 0:rows].astype(F32)
        for t in range(1, kinds):
            source = side(e, t, regions)
            if source is not None:
                total = total + recv[source, t * rows : (t + 1) * rows].astype(F32)
        parts.append(total)
    return jnp.concatenate(parts, axis=0)


def swap_lanes(values):
    half = values.shape[1] // 2
    return jnp.concatenate([values[:, half:], values[:, :half]], axis=1)


def departures(regions, rows, kinds, recv, pick):
    slots = gathered(regions, rows, kinds, recv)
    high = slots.astype(BF16).astype(F32)
    low = swap_lanes(slots - high)
    first = lax.broadcasted_iota(jnp.int32, slots.shape, 1) < slots.shape[1] // 2
    stacked = jnp.concatenate([jnp.where(first, high, low), jnp.where(first, low, high)], axis=0)
    found = dot(pick, stacked.astype(BF16))
    return found + swap_lanes(found)


def weigh(tiles, both):
    high = both.astype(BF16).astype(F32)
    first = lax.broadcasted_iota(jnp.int32, both.shape, 1) < both.shape[1] // 2
    split = jnp.where(first, high, both - high).astype(BF16)
    parts = []
    for i in range(tiles.shape[0]):
        own = split[i * TILE : (i + 1) * TILE]
        parts.append(dot(tiles[i], jnp.concatenate([own, own], axis=0)))
    out = jnp.concatenate(parts, axis=0)
    return out + swap_lanes(out)


def halves_apart(both):
    first = lax.broadcasted_iota(jnp.int32, both.shape, 1) < both.shape[1] // 2
    return jnp.concatenate([jnp.where(first, both, 0.0), jnp.where(first, 0.0, both)], axis=0).astype(BF16)


def column_sums(values):
    return jnp.sum(values.reshape(values.shape[0] // 8, 8, values.shape[1]), axis=0)


def weigh_kernel(regions, rows, kinds, recv, pick, pick_t, tiles, innov, out, dep_out, wgt_out, seen):
    dep = departures(regions, rows, kinds, recv, pick[...])
    if innov is not None:
        dep = dep - innov[...]
    wgt = weigh(tiles, dep)
    dep_out[...] = dep
    wgt_out[...] = wgt
    seen[...] = column_sums(0.5 * dep * wgt)
    back = dot(pick_t[...], halves_apart(wgt)).astype(BF16)
    for r in range(regions):
        for t in range(3):
            source = side(r, t, regions)
            if source is None:
                out[r, t * rows : (t + 1) * rows] = jnp.zeros((rows, back.shape[1]), BF16)
            else:
                out[r, t * rows : (t + 1) * rows] = back[source * rows : (source + 1) * rows]


def weigh_later_kernel(regions, rows, kinds, recv, pick, pick_t, tiles, out, dep_out, wgt_out, seen):
    weigh_kernel(regions, rows, kinds, recv, pick, pick_t, tiles, None, out, dep_out, wgt_out, seen)


def spread_regions(back, fill):
    regions = back.shape[0]
    tail = back.shape[1:]
    near = back.reshape((regions // 2, 2) + tail)[:, ::-1].reshape(back.shape)
    inner = back[1 : regions - 1].reshape((regions // 2 - 1, 2) + tail)[:, ::-1]
    blank = jnp.broadcast_to(fill, (1,) + tail)
    far = jnp.concatenate([blank, inner.reshape((regions - 2,) + tail), blank], axis=0)
    return jnp.concatenate([back, near, far], axis=1)


def weighed(regions, rows, recv, pick, pick_t, tiles, innov=None):
    lanes = recv.shape[2]
    kinds = recv.shape[1] // rows
    obs = pick.shape[0]
    if rows % 16:
        dep = departures(regions, rows, kinds, recv, pick)
        dep = dep if innov is None else dep - innov
        wgt = weigh(tiles, dep)
        back = dot(pick_t, halves_apart(wgt)).astype(BF16).reshape(regions, rows, lanes)
        return spread_regions(back, jnp.zeros((), BF16)), dep, wgt, column_sums(0.5 * dep * wgt)
    out = (
        shape((regions, 3 * rows, lanes), BF16),
        shape((obs, lanes), F32),
        shape((obs, lanes), F32),
        shape((8, lanes), F32),
    )
    args = [recv, pick, pick_t, tiles] + ([] if innov is None else [innov])
    kernel = weigh_later_kernel if innov is None else weigh_kernel
    return call(functools.partial(kernel, regions, rows, kinds), out, args)


def scattered_field(rows_t, onehot_t, lev):
    count = rows_t.shape[0]
    low = dot(onehot_t[:, :count], rows_t).T
    high = dot(onehot_t[:, count:], rows_t).T
    return low[:lev] + high[lev:]


def scatter_kernel(regions, rows, recv, onehot_t, out, half):
    lev = out.shape[2]
    for t in range(3):
        values = jnp.concatenate([recv[h, t * rows : (t + 1) * rows] for h in range(regions)], axis=0)
        field = scattered_field(values, onehot_t[t], lev)
        for s in range(SLOTS):
            piece = field[:, s * CELLS : (s + 1) * CELLS]
            out[t, s] = piece
            half[t, s] = piece.astype(BF16)


def scattered(regions, rows, recv, onehot_t):
    lanes = recv.shape[2]
    lev = lanes // 2
    if rows % 16:
        parts = []
        for t in range(3):
            values = recv[:, t * rows : (t + 1) * rows].reshape(regions * rows, lanes)
            field = scattered_field(values, onehot_t[t], lev)
            parts.append(jnp.stack([field[:, s * CELLS : (s + 1) * CELLS] for s in range(SLOTS)]))
        full = jnp.stack(parts)
        return full, full.astype(BF16)
    field = (3, SLOTS, lev, CELLS)
    return call(
        functools.partial(scatter_kernel, regions, rows),
        (shape(field, F32), shape(field, BF16)),
        [recv, onehot_t],
    )


def last_sums(regions, rows, recv, pick, tiles, dep, wgt, pieces, norms):
    total = jnp.sum(jnp.sum(pieces.astype(F32), axis=0), axis=0, keepdims=True)
    lane = lax.broadcasted_iota(jnp.int32, total.shape, 1)
    norm = jnp.sum(jnp.where(lane == 0, total, 0.0))
    seen = jnp.sum(jnp.where(lane == 1, total, 0.0))
    step = norm / (norm + seen)
    dep_image = departures(regions, rows, 3, recv, pick)
    dep_next = dep - step * dep_image
    wgt_next = weigh(tiles, dep_next)
    squares, mixed = norms(step)
    values = [
        squares,
        mixed,
        0.5 * jnp.sum(dep_next * wgt_next),
        0.5 * jnp.sum(dep_next * wgt),
    ]
    return scalar_row(values, 128), scalar_row([norm, seen, step], 128)


def last_kernel(regions, rows, group, recv, pick, tiles, dep, wgt, resid, image, out, known):
    count, lev, cells = resid.shape

    def norms(step):
        def add(g, carry):
            at = pl.ds(g * group, group)
            now = resid[at].reshape(group * lev, cells)
            later = now - step * image[at].reshape(group * lev, cells)
            return carry[0] + column_sums(later * later), carry[1] + column_sums(later * now)

        zero = jnp.zeros((8, cells), F32)
        squares, mixed = lax.fori_loop(0, count // group, add, (zero, zero))
        return jnp.sum(squares), jnp.sum(mixed)

    pieces = recv[:, 3 * rows : 3 * rows + 3]
    sums, facts = last_sums(regions, rows, recv, pick[...], tiles, dep[...], wgt[...], pieces, norms)
    wide = jnp.broadcast_to(sums, (8, 128))
    for r in range(regions):
        out[r] = wide
    known[...] = jnp.broadcast_to(facts, (8, 128))


def last(regions, rows, recv, pick, tiles, dep, wgt, resid, image):
    if rows % 16:

        def norms(step):
            later = resid - step * image
            return jnp.sum(later * later), jnp.sum(later * resid)

        sums, facts = last_sums(
            regions, rows, recv, pick, tiles, dep, wgt, recv[:, 3 * rows : 3 * rows + 3], norms
        )
        return jnp.broadcast_to(sums[None], (regions, 8, 128)), jnp.broadcast_to(facts, (8, 128))
    group = group_size(resid.shape[0])
    return call(
        functools.partial(last_kernel, regions, rows, group),
        (shape((regions, 8, 128), F32), shape((8, 128), F32)),
        [recv, pick, tiles, dep, wgt, resid, image],
    )


def finish(total, facts, emit):
    lane = lax.broadcasted_iota(jnp.int32, total.shape, 1)
    norm_next, mixed, seen_next, seen_mixed = (jnp.sum(jnp.where(lane == i, total, 0.0)) for i in range(4))
    norm, seen, step = (jnp.sum(jnp.where(lane == i, facts, 0.0)) for i in range(3))
    ratio = norm_next / norm
    curved = norm_next + seen_next + 2.0 * ratio * (mixed + seen_mixed) + ratio * ratio * (norm + seen)
    step_next = norm_next / curved
    along, across = step + step_next * (1.0 + ratio), step_next * step
    return emit(along, across)


def finish_kernel(group, sums, others, facts, control, resid, image, out):
    total = jnp.sum(sums[...] + others[...], axis=0)[0:1]

    def emit(along, across):
        def add(g, _):
            at = pl.ds(g * group, group)
            out[at] = control[at] + along * resid[at] - across * image[at]
            return 0

        lax.fori_loop(0, control.shape[0] // group, add, 0)

    finish(total, facts[0:1], emit)


def finished(sums, others, facts, control, resid, image):
    group = group_size(control.shape[0])
    return call(
        functools.partial(finish_kernel, group),
        jax.ShapeDtypeStruct(control.shape, F32),
        [sums, others, facts, control, resid, image],
    )


def to_regions(values):
    return lax.all_to_all(values, "region", split_axis=0, concat_axis=0, tiled=True)


def other_members(own, half):
    if lax.axis_size("member") == 2:
        return own, lax.ppermute(half, "member", [(0, 1), (1, 0)])
    return lax.psum(half, "member").astype(F32), jnp.zeros_like(half)


def member_sum(values):
    if lax.axis_size("member") == 2:
        return values + lax.ppermute(values, "member", [(0, 1), (1, 0)])
    return lax.psum(values, "member")


def local(
    perturbations,
    control,
    vertical_loc,
    block_kernels,
    loc_pattern,
    obs_region,
    obs_slot,
    obs_cell,
    innovations,
    obs_weight,
):
    regions = lax.axis_size("region")
    members = lax.axis_size("member")
    member = lax.axis_index("member")
    count, _, _ = control.shape
    obs = obs_region.shape[0] // members
    cap = max(2, 2 * obs // regions)

    chunks = HALO_CHUNKS if count % (4 * HALO_CHUNKS) == 0 else 1
    size = count // chunks
    group = group_size(size)

    near_p, far_p = halo([perturbations[i * size : (i + 1) * size] for i in range(chunks)])

    first = member * obs
    targets = lax.dynamic_slice_in_dim(obs_region[:, 0], first, obs, 0)
    codes = lax.dynamic_slice_in_dim(obs_slot * CELLS + obs_cell, first, obs, 0)
    named = targets[:, None] == jnp.arange(regions, dtype=jnp.int32)[None, :]
    lower = lax.broadcasted_iota(jnp.int32, (obs, obs), 0) > lax.broadcasted_iota(jnp.int32, (obs, obs), 1)
    earlier = dot(lower.astype(BF16), named.astype(BF16))
    rank = jnp.sum(jnp.where(named, earlier, 0.0), axis=1).astype(jnp.int32)
    rows = cap // 2
    slots_of_half = regions * rows
    position = (rank // rows) * slots_of_half + targets * rows + rank % rows
    slots = jnp.arange(2 * slots_of_half, dtype=jnp.int32)
    slot_codes = dot((slots[:, None] == position[None, :]).astype(BF16), (codes + 1).astype(BF16)[:, None])
    slot_codes = slot_codes[:, 0].astype(jnp.int32) - 1
    slot_codes = slot_codes.reshape(2, regions, rows).transpose(1, 0, 2)
    sent_codes = spread_regions(slot_codes, jnp.full((), -1, jnp.int32))
    sent_codes = jnp.pad(sent_codes, ((0, 0), (0, 2), (0, 128 - rows)))
    got_codes = to_regions(sent_codes)
    spots = jnp.broadcast_to(position[None], (8, obs))
    late = max(0, chunks - 2)
    got_codes, far_p[late] = lax.optimization_barrier((got_codes, far_p[late]))
    pick, pick_t, onehot, onehot_t, tiles, innov = select_all(
        rows, spots, got_codes, obs_weight, innovations
    )
    pick, far_p[-1] = lax.optimization_barrier((pick, far_p[-1]))

    own, lifted, tables, vert, vert_t = own_forward(
        loc_pattern, control, perturbations, block_kernels, vertical_loc, group
    )
    near, near_p = near_forward(near_p, lifted, tables, group)
    inc, half, far_p = far_forward(far_p, own, near, lifted, tables, group)
    inc, other = other_members(inc, half)
    recv = to_regions(sample(regions, rows, inc, other, onehot))
    back, _, _, _ = weighed(regions, rows, recv, pick, pick_t, tiles, innov)
    adj, adj_half = scattered(regions, rows, to_regions(back), onehot_t)
    adj, adj_other = other_members(adj, adj_half)
    resid, inc, half, square = turn(
        adj, adj_other, control, perturbations, near_p, far_p, tables, vert, vert_t, -1
    )

    inc, other = other_members(inc, half)
    recv = to_regions(sample(regions, rows, inc, other, onehot))
    back, dep, wgt, seen = weighed(regions, rows, recv, pick, pick_t, tiles)
    adj, adj_half = scattered(regions, rows, to_regions(back), onehot_t)
    adj, adj_other = other_members(adj, adj_half)
    square, seen = member_sum(square), member_sum(seen)
    image, inc, half, _ = turn(
        adj, adj_other, resid, perturbations, near_p, far_p, tables, vert, vert_t, 1
    )

    inc, other = other_members(inc, half)
    recv = to_regions(sample(regions, rows, inc, other, onehot, (square, seen)))
    sums, facts = last(regions, rows, recv, pick, tiles, dep, wgt, resid, image)
    sums, others = other_members(*[to_regions(sums)] * 2)
    return finished(sums, others, facts, control, resid, image)


def solution(mesh):
    placed = (
        P("member", None, None, "region"),
        P("member", None, "region"),
        P(),
        P(),
        P(),
        P("region", None),
        P("region"),
        P("region"),
        P(None, "region"),
        P("region", None, None),
    )

    return jax.shard_map(local, mesh=mesh, in_specs=placed, out_specs=P("member", None, "region"), check_vma=False)
```

```python
import functools

import jax
import jax.numpy as jnp
from jax import lax
from jax.experimental import pallas as pl
from jax.experimental.pallas import tpu as pltpu
from jax.sharding import PartitionSpec as P


SLOTS = 2
TILE = 128
CELLS = 128
CODES = SLOTS * CELLS
F32 = jnp.float32
BF16 = jnp.bfloat16
HALO_SHARES = (2, 3, 3, 2)


def near_of(r):
    return r ^ 1


def far_of(r, regions):
    other = r - 1 if r % 2 == 0 else r + 1
    return other if 0 <= other < regions else None


def side(r, t, regions):
    return (r, near_of(r), far_of(r, regions))[t]


def dot(a, b, dims=((1,), (0,)), precision=None):
    return lax.dot_general(a, b, (dims, ((), ())), precision=precision, preferred_element_type=F32)


def halo(chunks):
    regions = lax.axis_size("region")
    pairs = [(r, r ^ 1) for r in range(regions)]
    onward = [(r, r + 2 if r % 2 == 0 else r - 2) for r in range(regions)]
    onward = [(s, d) for s, d in onward if 0 <= d < regions]
    near, far = [], []
    for chunk in chunks:
        near.append(lax.ppermute(chunk, "region", pairs))
    for chunk in near:
        far.append(lax.ppermute(chunk, "region", onward))
    return near, far


def call(kernel, out_shape, args, scratch=(), limit=16, scalars=(), aliases=None):
    vmem = pl.BlockSpec(memory_space=pltpu.VMEM)
    return pl.pallas_call(
        kernel,
        out_shape=out_shape,
        in_specs=[pl.BlockSpec(memory_space=pltpu.SMEM)] * len(scalars) + [vmem] * len(args),
        out_specs=jax.tree.map(lambda _: vmem, out_shape),
        scratch_shapes=list(scratch),
        input_output_aliases=aliases or {},
        compiler_params=pltpu.CompilerParams(vmem_limit_bytes=limit << 20),
    )(*scalars, *[pltpu.with_memory_space_constraint(a, pltpu.VMEM) for a in args])


def halo_sizes(groups):
    whole = sum(HALO_SHARES)
    ends = sorted({max(1, groups * sum(HALO_SHARES[: i + 1]) // whole) for i in range(len(HALO_SHARES))})
    if len(ends) < 2:
        ends = [1, groups]
    return [b - a for a, b in zip([0] + ends, ends)]


def group_size(members):
    return 4 if members % 4 == 0 else 2 if members % 2 == 0 else 1


def shape(dims, dtype):
    return pltpu.VMEM(dims, dtype)


def block_diagonal(matrix, copies, transposed):
    size = matrix.shape[0]
    total = copies * size
    row = lax.broadcasted_iota(jnp.int32, (total, size), 0)
    place = (row % size == lax.broadcasted_iota(jnp.int32, (total, size), 1)).astype(BF16)
    tall = dot(place, matrix, ((1,), (1 if transposed else 0,))).astype(BF16)
    wide = dot(tall, place, ((1,), (1,)))
    same = (
        lax.broadcasted_iota(jnp.int32, (total, total), 0) // size
        == lax.broadcasted_iota(jnp.int32, (total, total), 1) // size
    )
    return jnp.where(same, wide, 0.0).astype(BF16)


def own_kernel(group, pattern, start, pert, kernels, vloc, inc, lifted, tables, vert, vert_t, acc):
    count, lev, _ = start.shape
    rows = group * lev
    acc[...] = jnp.zeros_like(acc)
    vert[...] = block_diagonal(vloc[...], group, False)
    vert_t[...] = block_diagonal(vloc[...], group, True)
    region = lax.axis_index("region")
    even = region % 2 == 0
    up = pattern[jnp.minimum(region + 1, pattern.shape[0] - 1), 0]
    down = pattern[jnp.maximum(region - 1, 0), 2]
    picks = (pattern[region, 1], jnp.where(even, up, down), jnp.where(even, down, up))
    for t in range(3):
        tables[:, t * CELLS : (t + 1) * CELLS] = kernels[picks[t]]

    def mix(g):
        at = pl.ds(g * group, group)
        mixed = dot(vert[...], start[at].reshape(rows, CELLS).astype(BF16)).astype(BF16)
        lifted[at] = mixed.reshape(group, lev, CELLS)

    def gather(g):
        at = pl.ds(g * group, group)
        local = dot(lifted[at].reshape(rows, CELLS), tables[:, :CELLS])
        values = pert[at]
        for s in range(SLOTS):
            total = acc[s]
            for j in range(group):
                total += values[j, s].astype(F32) * local[j * lev : (j + 1) * lev]
            acc[s] = total

    def step(g, _):
        gather(g - 1)
        mix(g)
        return 0

    steps = count // group
    mix(0)
    lax.fori_loop(1, steps, step, 0, unroll=3 if steps % 3 == 1 else 1)
    gather(steps - 1)
    inc[...] = acc[...]


def own_forward(pattern, start, pert, kernels, vloc, group):
    _, lev, _ = start.shape
    field = (SLOTS, lev, CELLS)
    square = shape((group * lev, group * lev), BF16)
    out = (shape(field, F32), shape(start.shape, BF16), shape((CELLS, 3 * CELLS), BF16), square, square)
    return call(
        functools.partial(own_kernel, group),
        out,
        [start, pert, kernels, vloc],
        [pltpu.VMEM(field, F32)],
        scalars=[pattern],
    )


def part_sum(first, group, t, chunks, lifted, tables, acc, full):
    lev = lifted.shape[1]
    rows = group * lev
    for chunk in chunks:
        size = chunk.shape[0]

        def step(g, _, chunk=chunk, first=first):
            at = pl.ds(first + g * group, group)
            local = dot(lifted[at].reshape(rows, CELLS), tables[:, t * CELLS : (t + 1) * CELLS])
            values = chunk[pl.ds(g * group, group)]
            full[at] = values
            for s in range(SLOTS):
                total = acc[s]
                for j in range(group):
                    total += values[j, s].astype(F32) * local[j * lev : (j + 1) * lev]
                acc[s] = total
            return 0

        lax.fori_loop(0, size // group, step, 0, unroll=size // group)
        first += size


def begin_kernel(n, group, t, *refs):
    chunks = refs[:n]
    lifted, tables, inc, full = refs[n:]
    inc[...] = jnp.zeros_like(inc)
    part_sum(0, group, t, chunks, lifted, tables, inc, full)


def begin_part(chunks, t, lifted, tables, group):
    count, lev, cells = lifted.shape
    out = (shape((SLOTS, lev, cells), F32), shape((count,) + chunks[0].shape[1:], chunks[0].dtype))
    return call(functools.partial(begin_kernel, len(chunks), group, t), out, [*chunks, lifted, tables])


def end_kernel(first, group, full_in, chunk, own, near, begun, lifted, tables, full, inc, half, acc):
    del full_in
    acc[...] = begun[...]
    if chunk is not None:
        part_sum(first, group, 2, [chunk], lifted, tables, acc, full)
    for t, part in enumerate((own, near, acc)):
        inc[t] = part[...]
        half[t] = part[...].astype(BF16)


def end_parts(chunk, own, near, begun, full, lifted, tables, group):
    count, lev, cells = lifted.shape
    field = (SLOTS, lev, cells)
    out = (shape(full.shape, full.dtype), shape((3,) + field, F32), shape((3,) + field, BF16))
    args = [full, chunk, own, near, begun, lifted, tables]
    kernel = functools.partial(end_kernel, count - chunk.shape[0], group)
    return call(kernel, out, args, [pltpu.VMEM(field, F32)], aliases={0: 0})


def columns(row, width):
    return jnp.broadcast_to(row.astype(F32), (width, row.shape[1])).T.astype(jnp.int32)


def lane_choice(column, start, width):
    lanes = lax.broadcasted_iota(jnp.int32, column.shape, 1)
    blocks = [jnp.where(column == lanes + (start + b), 1.0, 0.0).astype(BF16) for b in range(0, width, column.shape[1])]
    return blocks[0] if len(blocks) == 1 else jnp.concatenate(blocks, axis=1)


def row_choice(row, start, count):
    index = lax.broadcasted_iota(jnp.int32, (count, row.shape[1]), 0) + start
    return jnp.where(index == row, 1.0, 0.0).astype(BF16)


def code_rows(recv, rows):
    return [
        jnp.concatenate([recv[h, k : k + 1, :rows] for h in range(recv.shape[0])], axis=1) for k in range(6)
    ]


def selections(position, codes, weight, innov):
    half = codes[0].shape[1]
    column = columns(position, 128)
    pick = lane_choice(column, 0, 2 * half)
    pick_t = jnp.concatenate([row_choice(position, i * half, half) for i in range(2)], axis=1)
    onehot, onehot_t = [], []
    for t in range(3):
        pair = codes[2 * t : 2 * t + 2]
        onehot.append(jnp.concatenate([lane_choice(columns(row, 128), 0, CODES) for row in pair], axis=1))
        onehot_t.append(jnp.concatenate([row_choice(row, 0, CODES) for row in pair], axis=1))
    high = weight.astype(BF16)
    tiles = jnp.concatenate([high, (weight - high.astype(F32)).astype(BF16)], axis=2)
    turned = innov.T
    return pick, pick_t, onehot, onehot_t, tiles, jnp.concatenate([turned, turned], axis=1)


def selections_kernel(rows, position, codes, weight, innov, pick, pick_t, onehot, onehot_t, tiles, turned):
    obs = position.shape[1]
    member = lax.axis_index("member")
    kept = weight[pl.ds(member * (obs // TILE), obs // TILE)]
    seen = innov[:, pl.ds(pl.multiple_of(member * obs, obs), obs)]
    made = selections(position[0:1], code_rows(codes, rows), kept, seen)
    pick[...], pick_t[...] = made[0], made[1]
    for t in range(3):
        onehot[t], onehot_t[t] = made[2][t], made[3][t]
    tiles[...], turned[...] = made[4], made[5]


def select_all(rows, position, codes, weight, innov):
    obs = position.shape[1]
    half = codes.shape[0] * rows
    if rows % 16:
        member = lax.axis_index("member")
        kept = lax.dynamic_slice_in_dim(weight, member * (obs // TILE), obs // TILE, 0)
        seen = lax.dynamic_slice_in_dim(innov, member * obs, obs, 1)
        pick, pick_t, onehot, onehot_t, tiles, turned = selections(
            position[0:1], code_rows(codes, rows), kept, seen
        )
        return pick, pick_t, jnp.stack(onehot), jnp.stack(onehot_t), tiles, turned
    lev = innov.shape[0]
    out = (
        shape((obs, 2 * half), BF16),
        shape((half, 2 * obs), BF16),
        shape((3, half, 2 * CODES), BF16),
        shape((3, CODES, 2 * half), BF16),
        shape((obs // TILE, TILE, 2 * TILE), BF16),
        shape((obs, 2 * lev), F32),
    )
    return call(functools.partial(selections_kernel, rows), out, [position, codes, weight, innov])


def turn_kernel(group, sign, *refs):
    near, far, adj_own, adj_other, base, pert, tables, vert, vert_t, vec, inc, inc_half, square = refs[:13]
    adj, acc, moved, mixed = refs[13:]
    rows = vert.shape[0]
    lev = rows // group
    adj[...] = adj_own[...] + adj_other[...].astype(F32)
    acc[...] = jnp.zeros_like(acc)
    square[...] = jnp.zeros_like(square)
    sources = (pert, near, far)

    def project(g):
        parts = []
        for t in range(3):
            values = sources[t][pl.ds(g * group, group)].astype(F32)
            parts.append(
                jnp.concatenate(
                    [(values[j, 0] * adj[t, 0] + values[j, 1] * adj[t, 1]).astype(BF16) for j in range(group)],
                    axis=0,
                )
            )
        moved[g] = dot(jnp.concatenate(parts, axis=1), tables[...], ((1,), (1,))).astype(BF16)

    def lift(g):
        at = pl.ds(g * group, group)
        new = base[at].reshape(rows, CELLS) + dot(vert_t[...], moved[g])
        if sign < 0:
            new = -new
        vec[at] = new.reshape(group, lev, CELLS)
        square[...] += jnp.sum((new * new).reshape(rows // 8, 8, CELLS), axis=0)

    def mix(g):
        half = vec[pl.ds(g * group, group)].reshape(rows, CELLS).astype(BF16)
        mixed[g] = dot(vert[...], half).astype(BF16)

    def gather(g):
        local = dot(mixed[g], tables[...])
        for t in range(3):
            values = sources[t][pl.ds(g * group, group)]
            for s in range(SLOTS):
                total = acc[t, s]
                for j in range(group):
                    part = local[j * lev : (j + 1) * lev, t * CELLS : (t + 1) * CELLS]
                    total += values[j, s].astype(F32) * part
                acc[t, s] = total

    stages = (gather, mix, lift, project)
    steps = base.shape[0] // group
    depth = len(stages)
    for i in range(min(depth - 1, steps)):
        for k, stage in enumerate(stages):
            if 0 <= i - (depth - 1 - k):
                stage(i - (depth - 1 - k))

    def step(g, _):
        for k, stage in enumerate(stages):
            stage(g - (depth - 1 - k))
        return 0

    lax.fori_loop(depth - 1, steps, step, 0)
    for i in range(max(steps, depth - 1), steps + depth - 1):
        for k, stage in enumerate(stages):
            if 0 <= i - (depth - 1 - k) < steps:
                stage(i - (depth - 1 - k))
    inc[...] = acc[...]
    inc_half[...] = acc[...].astype(BF16)


def turn(adj_own, adj_other, base, pert, near, far, tables, vert, vert_t, sign):
    count, lev, _ = base.shape
    group = vert.shape[0] // lev
    field = (3, SLOTS, lev, CELLS)
    out = (shape(base.shape, F32), shape(field, F32), shape(field, BF16), shape((8, CELLS), F32))
    half = pltpu.VMEM((count // group, group * lev, CELLS), BF16)
    return call(
        functools.partial(turn_kernel, group, sign),
        out,
        [near, far, adj_own, adj_other, base, pert, tables, vert, vert_t],
        [pltpu.VMEM(field, F32), pltpu.VMEM(field, F32), half, half],
    )


def three_pieces(row, rows):
    high = row.astype(BF16).astype(F32)
    mid = (row - high).astype(BF16).astype(F32)
    low = row - high - mid
    index = lax.broadcasted_iota(jnp.int32, (rows, row.shape[1]), 0)
    tile = jnp.where(index == 0, high, jnp.where(index == 1, mid, jnp.where(index == 2, low, 0.0)))
    return tile.astype(BF16)


def twice(cells):
    blank = jnp.zeros_like(cells)
    return jnp.concatenate(
        [jnp.concatenate([cells, blank], axis=1), jnp.concatenate([blank, cells], axis=1)], axis=0
    )


def scalar_row(values, width):
    lane = lax.broadcasted_iota(jnp.int32, (1, width), 1)
    row = jnp.zeros((1, width), F32)
    for i, value in enumerate(values):
        row = jnp.where(lane == i, value, row)
    return row


def sampled_rows(inc, other, onehot, t):
    total = (inc[t] + other[t].astype(F32)).astype(BF16)
    cells = jnp.concatenate([total[s] for s in range(SLOTS)], axis=1)
    return dot(onehot[t], twice(cells), ((1,), (1,))).astype(BF16)


def sample_kernel(regions, rows, kinds, inc, other, onehot, *refs):
    out = refs[-1]
    for t in range(kinds):
        found = sampled_rows(inc, other, onehot, t)
        for h in range(regions):
            out[h, t * rows : (t + 1) * rows] = found[h * rows : (h + 1) * rows]
    if len(refs) > 1:
        tile = three_pieces(scalar_row([jnp.sum(ref[...]) for ref in refs[:-1]], out.shape[2]), 8)
        for h in range(regions):
            out[h, kinds * rows :] = tile


def sample(regions, rows, inc, other, onehot, scal=()):
    kinds, lev = inc.shape[0], inc.shape[2]
    extra = 8 if scal else 0
    if rows % 16:
        parts = [sampled_rows(inc, other, onehot, t).reshape(regions, rows, 2 * lev) for t in range(kinds)]
        if scal:
            tile = three_pieces(scalar_row([jnp.sum(v) for v in scal], 2 * lev), 8)
            parts.append(jnp.broadcast_to(tile[None], (regions,) + tile.shape))
        return jnp.concatenate(parts, axis=1)
    return call(
        functools.partial(sample_kernel, regions, rows, kinds),
        shape((regions, kinds * rows + extra, 2 * lev), BF16),
        [inc, other, onehot, *scal],
    )


def gathered(regions, rows, kinds, recv):
    parts = []
    for e in range(regions):
        total = recv[e, 0:rows].astype(F32)
        for t in range(1, kinds):
            source = side(e, t, regions)
            if source is not None:
                total = total + recv[source, t * rows : (t + 1) * rows].astype(F32)
        parts.append(total)
    return jnp.concatenate(parts, axis=0)


def swap_lanes(values):
    half = values.shape[1] // 2
    return jnp.concatenate([values[:, half:], values[:, :half]], axis=1)


def departures(regions, rows, kinds, recv, pick):
    slots = gathered(regions, rows, kinds, recv)
    high = slots.astype(BF16).astype(F32)
    low = swap_lanes(slots - high)
    first = lax.broadcasted_iota(jnp.int32, slots.shape, 1) < slots.shape[1] // 2
    stacked = jnp.concatenate([jnp.where(first, high, low), jnp.where(first, low, high)], axis=0)
    found = dot(pick, stacked.astype(BF16))
    return found + swap_lanes(found)


def weigh(tiles, both):
    high = both.astype(BF16).astype(F32)
    first = lax.broadcasted_iota(jnp.int32, both.shape, 1) < both.shape[1] // 2
    split = jnp.where(first, high, both - high).astype(BF16)
    parts = []
    for i in range(tiles.shape[0]):
        own = split[i * TILE : (i + 1) * TILE]
        parts.append(dot(tiles[i], jnp.concatenate([own, own], axis=0)))
    out = jnp.concatenate(parts, axis=0)
    return out + swap_lanes(out)


def halves_apart(both):
    first = lax.broadcasted_iota(jnp.int32, both.shape, 1) < both.shape[1] // 2
    return jnp.concatenate([jnp.where(first, both, 0.0), jnp.where(first, 0.0, both)], axis=0).astype(BF16)


def column_sums(values):
    return jnp.sum(values.reshape(values.shape[0] // 8, 8, values.shape[1]), axis=0)


def weigh_kernel(regions, rows, kinds, recv, pick, pick_t, tiles, innov, out, dep_out, wgt_out, seen):
    dep = departures(regions, rows, kinds, recv, pick[...])
    if innov is not None:
        dep = dep - innov[...]
    wgt = weigh(tiles, dep)
    dep_out[...] = dep
    wgt_out[...] = wgt
    seen[...] = column_sums(0.5 * dep * wgt)
    back = dot(pick_t[...], halves_apart(wgt)).astype(BF16)
    for r in range(regions):
        for t in range(3):
            source = side(r, t, regions)
            if source is None:
                out[r, t * rows : (t + 1) * rows] = jnp.zeros((rows, back.shape[1]), BF16)
            else:
                out[r, t * rows : (t + 1) * rows] = back[source * rows : (source + 1) * rows]


def weigh_later_kernel(regions, rows, kinds, recv, pick, pick_t, tiles, out, dep_out, wgt_out, seen):
    weigh_kernel(regions, rows, kinds, recv, pick, pick_t, tiles, None, out, dep_out, wgt_out, seen)


def spread_regions(back, fill):
    regions = back.shape[0]
    tail = back.shape[1:]
    near = back.reshape((regions // 2, 2) + tail)[:, ::-1].reshape(back.shape)
    inner = back[1 : regions - 1].reshape((regions // 2 - 1, 2) + tail)[:, ::-1]
    blank = jnp.broadcast_to(fill, (1,) + tail)
    far = jnp.concatenate([blank, inner.reshape((regions - 2,) + tail), blank], axis=0)
    return jnp.concatenate([back, near, far], axis=1)


def weighed(regions, rows, recv, pick, pick_t, tiles, innov=None):
    lanes = recv.shape[2]
    kinds = recv.shape[1] // rows
    obs = pick.shape[0]
    if rows % 16:
        dep = departures(regions, rows, kinds, recv, pick)
        dep = dep if innov is None else dep - innov
        wgt = weigh(tiles, dep)
        back = dot(pick_t, halves_apart(wgt)).astype(BF16).reshape(regions, rows, lanes)
        return spread_regions(back, jnp.zeros((), BF16)), dep, wgt, column_sums(0.5 * dep * wgt)
    out = (
        shape((regions, 3 * rows, lanes), BF16),
        shape((obs, lanes), F32),
        shape((obs, lanes), F32),
        shape((8, lanes), F32),
    )
    args = [recv, pick, pick_t, tiles] + ([] if innov is None else [innov])
    kernel = weigh_later_kernel if innov is None else weigh_kernel
    return call(functools.partial(kernel, regions, rows, kinds), out, args)


def scattered_field(rows_t, onehot_t, lev):
    count = rows_t.shape[0]
    low = dot(onehot_t[:, :count], rows_t).T
    high = dot(onehot_t[:, count:], rows_t).T
    return low[:lev] + high[lev:]


def scatter_kernel(regions, rows, recv, onehot_t, out, half):
    lev = out.shape[2]
    for t in range(3):
        values = jnp.concatenate([recv[h, t * rows : (t + 1) * rows] for h in range(regions)], axis=0)
        field = scattered_field(values, onehot_t[t], lev)
        for s in range(SLOTS):
            piece = field[:, s * CELLS : (s + 1) * CELLS]
            out[t, s] = piece
            half[t, s] = piece.astype(BF16)


def scattered(regions, rows, recv, onehot_t):
    lanes = recv.shape[2]
    lev = lanes // 2
    if rows % 16:
        parts = []
        for t in range(3):
            values = recv[:, t * rows : (t + 1) * rows].reshape(regions * rows, lanes)
            field = scattered_field(values, onehot_t[t], lev)
            parts.append(jnp.stack([field[:, s * CELLS : (s + 1) * CELLS] for s in range(SLOTS)]))
        full = jnp.stack(parts)
        return full, full.astype(BF16)
    field = (3, SLOTS, lev, CELLS)
    return call(
        functools.partial(scatter_kernel, regions, rows),
        (shape(field, F32), shape(field, BF16)),
        [recv, onehot_t],
    )


def last_sums(regions, rows, recv, pick, tiles, dep, wgt, pieces, norms):
    total = jnp.sum(jnp.sum(pieces.astype(F32), axis=0), axis=0, keepdims=True)
    lane = lax.broadcasted_iota(jnp.int32, total.shape, 1)
    norm = jnp.sum(jnp.where(lane == 0, total, 0.0))
    seen = jnp.sum(jnp.where(lane == 1, total, 0.0))
    step = norm / (norm + seen)
    dep_image = departures(regions, rows, 3, recv, pick)
    dep_next = dep - step * dep_image
    wgt_next = weigh(tiles, dep_next)
    squares, mixed = norms(step)
    values = [
        squares,
        mixed,
        0.5 * jnp.sum(dep_next * wgt_next),
        0.5 * jnp.sum(dep_next * wgt),
    ]
    return scalar_row(values, 128), scalar_row([norm, seen, step], 128)


def last_kernel(regions, rows, group, recv, pick, tiles, dep, wgt, resid, image, out, known):
    count, lev, cells = resid.shape

    def norms(step):
        def add(g, carry):
            at = pl.ds(g * group, group)
            now = resid[at].reshape(group * lev, cells)
            later = now - step * image[at].reshape(group * lev, cells)
            return carry[0] + column_sums(later * later), carry[1] + column_sums(later * now)

        zero = jnp.zeros((8, cells), F32)
        squares, mixed = lax.fori_loop(0, count // group, add, (zero, zero))
        return jnp.sum(squares), jnp.sum(mixed)

    pieces = recv[:, 3 * rows : 3 * rows + 3]
    sums, facts = last_sums(regions, rows, recv, pick[...], tiles, dep[...], wgt[...], pieces, norms)
    wide = jnp.broadcast_to(sums, (8, 128))
    for r in range(regions):
        out[r] = wide
    known[...] = jnp.broadcast_to(facts, (8, 128))


def last(regions, rows, recv, pick, tiles, dep, wgt, resid, image):
    if rows % 16:

        def norms(step):
            later = resid - step * image
            return jnp.sum(later * later), jnp.sum(later * resid)

        sums, facts = last_sums(
            regions, rows, recv, pick, tiles, dep, wgt, recv[:, 3 * rows : 3 * rows + 3], norms
        )
        return jnp.broadcast_to(sums[None], (regions, 8, 128)), jnp.broadcast_to(facts, (8, 128))
    group = group_size(resid.shape[0])
    return call(
        functools.partial(last_kernel, regions, rows, group),
        (shape((regions, 8, 128), F32), shape((8, 128), F32)),
        [recv, pick, tiles, dep, wgt, resid, image],
    )


def finish(total, facts, emit):
    lane = lax.broadcasted_iota(jnp.int32, total.shape, 1)
    norm_next, mixed, seen_next, seen_mixed = (jnp.sum(jnp.where(lane == i, total, 0.0)) for i in range(4))
    norm, seen, step = (jnp.sum(jnp.where(lane == i, facts, 0.0)) for i in range(3))
    ratio = norm_next / norm
    curved = norm_next + seen_next + 2.0 * ratio * (mixed + seen_mixed) + ratio * ratio * (norm + seen)
    step_next = norm_next / curved
    along, across = step + step_next * (1.0 + ratio), step_next * step
    return emit(along, across)


def finish_kernel(group, sums, others, facts, control, resid, image, out):
    total = jnp.sum(sums[...] + others[...], axis=0)[0:1]

    def emit(along, across):
        def add(g, _):
            at = pl.ds(g * group, group)
            out[at] = control[at] + along * resid[at] - across * image[at]
            return 0

        lax.fori_loop(0, control.shape[0] // group, add, 0)

    finish(total, facts[0:1], emit)


def finished(sums, others, facts, control, resid, image):
    group = group_size(control.shape[0])
    return call(
        functools.partial(finish_kernel, group),
        jax.ShapeDtypeStruct(control.shape, F32),
        [sums, others, facts, control, resid, image],
    )


def to_regions(values):
    return lax.all_to_all(values, "region", split_axis=0, concat_axis=0, tiled=True)


def other_members(own, half):
    if lax.axis_size("member") == 2:
        return own, lax.ppermute(half, "member", [(0, 1), (1, 0)])
    return lax.psum(half, "member").astype(F32), jnp.zeros_like(half)


def member_sum(values):
    if lax.axis_size("member") == 2:
        return values + lax.ppermute(values, "member", [(0, 1), (1, 0)])
    return lax.psum(values, "member")


def local(
    perturbations,
    control,
    vertical_loc,
    block_kernels,
    loc_pattern,
    obs_region,
    obs_slot,
    obs_cell,
    innovations,
    obs_weight,
):
    regions = lax.axis_size("region")
    members = lax.axis_size("member")
    member = lax.axis_index("member")
    count, _, _ = control.shape
    obs = obs_region.shape[0] // members
    cap = max(2, 2 * obs // regions)

    group = group_size(count)
    sizes = halo_sizes(count // group)
    starts = [sum(sizes[:i]) * group for i in range(len(sizes) + 1)]
    rest = lax.optimization_barrier(perturbations)
    pieces = [(rest if i else perturbations)[starts[i] : starts[i + 1]] for i in range(len(sizes))]
    near_p, far_p = halo(pieces)

    first = member * obs
    targets = lax.dynamic_slice_in_dim(obs_region[:, 0], first, obs, 0)
    codes = lax.dynamic_slice_in_dim(obs_slot * CELLS + obs_cell, first, obs, 0)
    named = targets[:, None] == jnp.arange(regions, dtype=jnp.int32)[None, :]
    lower = lax.broadcasted_iota(jnp.int32, (obs, obs), 0) > lax.broadcasted_iota(jnp.int32, (obs, obs), 1)
    earlier = dot(lower.astype(BF16), named.astype(BF16))
    rank = jnp.sum(jnp.where(named, earlier, 0.0), axis=1).astype(jnp.int32)
    rows = cap // 2
    slots_of_half = regions * rows
    position = (rank // rows) * slots_of_half + targets * rows + rank % rows
    slots = jnp.arange(2 * slots_of_half, dtype=jnp.int32)
    slot_codes = dot((slots[:, None] == position[None, :]).astype(BF16), (codes + 1).astype(BF16)[:, None])
    slot_codes = slot_codes[:, 0].astype(jnp.int32) - 1
    slot_codes = slot_codes.reshape(2, regions, rows).transpose(1, 0, 2)
    sent_codes = spread_regions(slot_codes, jnp.full((), -1, jnp.int32))
    sent_codes = jnp.pad(sent_codes, ((0, 0), (0, 2), (0, 128 - rows)))
    got_codes = to_regions(sent_codes)
    spots = jnp.broadcast_to(position[None], (8, obs))
    got_codes, loc_pattern = lax.optimization_barrier((got_codes, loc_pattern))
    pick, pick_t, onehot, onehot_t, tiles, innov = select_all(
        rows, spots, got_codes, obs_weight, innovations
    )
    pick, far_p[-1] = lax.optimization_barrier((pick, far_p[-1]))

    own, lifted, tables, vert, vert_t = own_forward(
        loc_pattern, control, perturbations, block_kernels, vertical_loc, group
    )
    near, near_p = begin_part(near_p, 1, lifted, tables, group)
    begun, joined = begin_part(far_p[:-1], 2, lifted, tables, group)
    far_p, inc, half = end_parts(far_p[-1], own, near, begun, joined, lifted, tables, group)
    inc, other = other_members(inc, half)
    recv = to_regions(sample(regions, rows, inc, other, onehot))
    back, _, _, _ = weighed(regions, rows, recv, pick, pick_t, tiles, innov)
    adj, adj_half = scattered(regions, rows, to_regions(back), onehot_t)
    adj, adj_other = other_members(adj, adj_half)
    resid, inc, half, square = turn(
        adj, adj_other, control, perturbations, near_p, far_p, tables, vert, vert_t, -1
    )

    inc, other = other_members(inc, half)
    recv = to_regions(sample(regions, rows, inc, other, onehot))
    back, dep, wgt, seen = weighed(regions, rows, recv, pick, pick_t, tiles)
    adj, adj_half = scattered(regions, rows, to_regions(back), onehot_t)
    adj, adj_other = other_members(adj, adj_half)
    square, seen = member_sum(square), member_sum(seen)
    image, inc, half, _ = turn(
        adj, adj_other, resid, perturbations, near_p, far_p, tables, vert, vert_t, 1
    )

    inc, other = other_members(inc, half)
    recv = to_regions(sample(regions, rows, inc, other, onehot, (square, seen)))
    sums, facts = last(regions, rows, recv, pick, tiles, dep, wgt, resid, image)
    sums, others = other_members(*[to_regions(sums)] * 2)
    return finished(sums, others, facts, control, resid, image)


def solution(mesh):
    placed = (
        P("member", None, None, "region"),
        P("member", None, "region"),
        P(),
        P(),
        P(),
        P("region", None),
        P("region"),
        P("region"),
        P(None, "region"),
        P("region", None, None),
    )

    return jax.shard_map(local, mesh=mesh, in_specs=placed, out_specs=P("member", None, "region"), check_vma=False)
```

```python
import functools

import jax
import jax.numpy as jnp
from jax import lax
from jax.experimental import pallas as pl
from jax.experimental.pallas import tpu as pltpu
from jax.sharding import PartitionSpec as P


SLOTS = 2
TILE = 128
CELLS = 128
CODES = SLOTS * CELLS
F32 = jnp.float32
BF16 = jnp.bfloat16
HALO_SHARES = (3, 3, 2, 2)


def near_of(r):
    return r ^ 1


def far_of(r, regions):
    other = r - 1 if r % 2 == 0 else r + 1
    return other if 0 <= other < regions else None


def side(r, t, regions):
    return (r, near_of(r), far_of(r, regions))[t]


def dot(a, b, dims=((1,), (0,)), precision=None):
    return lax.dot_general(a, b, (dims, ((), ())), precision=precision, preferred_element_type=F32)


def halo(chunks):
    regions = lax.axis_size("region")
    pairs = [(r, r ^ 1) for r in range(regions)]
    onward = [(r, r + 2 if r % 2 == 0 else r - 2) for r in range(regions)]
    onward = [(s, d) for s, d in onward if 0 <= d < regions]
    near, far = [], []
    for chunk in chunks:
        near.append(lax.ppermute(chunk, "region", pairs))
    for chunk in near:
        far.append(lax.ppermute(chunk, "region", onward))
    return near, far


def call(kernel, out_shape, args, scratch=(), limit=16, scalars=(), aliases=None):
    vmem = pl.BlockSpec(memory_space=pltpu.VMEM)
    return pl.pallas_call(
        kernel,
        out_shape=out_shape,
        in_specs=[pl.BlockSpec(memory_space=pltpu.SMEM)] * len(scalars) + [vmem] * len(args),
        out_specs=jax.tree.map(lambda _: vmem, out_shape),
        scratch_shapes=list(scratch),
        input_output_aliases=aliases or {},
        compiler_params=pltpu.CompilerParams(vmem_limit_bytes=limit << 20),
    )(*scalars, *[pltpu.with_memory_space_constraint(a, pltpu.VMEM) for a in args])


def halo_sizes(groups):
    whole = sum(HALO_SHARES)
    ends = sorted({max(1, groups * sum(HALO_SHARES[: i + 1]) // whole) for i in range(len(HALO_SHARES))})
    if len(ends) < 2:
        ends = [1, groups]
    return [b - a for a, b in zip([0] + ends, ends)]


def group_size(members):
    return 4 if members % 4 == 0 else 2 if members % 2 == 0 else 1


def shape(dims, dtype):
    return pltpu.VMEM(dims, dtype)


def block_diagonal(matrix, copies, transposed):
    side_by_side = jnp.concatenate([matrix] * copies, axis=0)
    size, total = matrix.shape[0], copies * matrix.shape[0]
    index = lax.broadcasted_iota(jnp.int32, (size, total), 0)
    lane = lax.broadcasted_iota(jnp.int32, (size, total), 1)
    parts = []
    for i in range(copies):
        place = (lane == index + i * size).astype(BF16)
        part = side_by_side[i * size : (i + 1) * size]
        parts.append(dot(part, place, ((0 if transposed else 1,), (0,))).astype(BF16))
    return jnp.concatenate(parts, axis=0)


def own_kernel(group, pattern, start, pert, kernels, vloc, inc, lifted, tables, vert, vert_t):
    count, lev, _ = start.shape
    rows = group * lev
    vert[...] = block_diagonal(vloc[...], group, False)
    vert_t[...] = block_diagonal(vloc[...], group, True)
    region = lax.axis_index("region")
    even = region % 2 == 0
    up = pattern[0, jnp.minimum(region + 1, pattern.shape[1] - 1)]
    down = pattern[2, jnp.maximum(region - 1, 0)]
    picks = (pattern[1, region], jnp.where(even, up, down), jnp.where(even, down, up))
    for t in range(3):
        tables[:, t * CELLS : (t + 1) * CELLS] = kernels[picks[t]]

    def mix(g):
        at = pl.ds(g * group, group)
        mixed = dot(vert[...], start[at].reshape(rows, CELLS).astype(BF16)).astype(BF16)
        lifted[at] = mixed.reshape(group, lev, CELLS)

    def gather(g):
        at = pl.ds(g * group, group)
        local = dot(lifted[at].reshape(rows, CELLS), tables[:, :CELLS])
        values = pert[at]
        for s in range(SLOTS):
            for j in range(group):
                totals[s] = totals[s] + values[j, s].astype(F32) * local[j * lev : (j + 1) * lev]

    steps = count // group
    totals = [jnp.zeros((lev, CELLS), F32)] * SLOTS
    mix(0)
    for g in range(1, steps):
        mix(g)
        gather(g - 1)
    gather(steps - 1)
    for s in range(SLOTS):
        inc[s] = totals[s]


def own_forward(pattern, start, pert, kernels, vloc, group):
    _, lev, _ = start.shape
    field = (SLOTS, lev, CELLS)
    square = shape((group * lev, group * lev), BF16)
    out = (shape(field, F32), shape(start.shape, BF16), shape((CELLS, 3 * CELLS), BF16), square, square)
    return call(
        functools.partial(own_kernel, group),
        out,
        [start, pert, kernels, vloc],
        scalars=[pattern],
    )


def part_sum(first, group, t, chunks, lifted, tables, acc, full):
    lev = lifted.shape[1]
    rows = group * lev
    totals = [acc[s] for s in range(SLOTS)]
    for chunk in chunks:
        for g in range(chunk.shape[0] // group):
            at = slice(first + g * group, first + (g + 1) * group)
            local = dot(lifted[at].reshape(rows, CELLS), tables[:, t * CELLS : (t + 1) * CELLS])
            values = chunk[g * group : (g + 1) * group]
            full[at] = values
            for s in range(SLOTS):
                for j in range(group):
                    totals[s] = totals[s] + values[j, s].astype(F32) * local[j * lev : (j + 1) * lev]
        first += chunk.shape[0]
    for s in range(SLOTS):
        acc[s] = totals[s]


def begin_kernel(n, group, t, *refs):
    chunks = refs[:n]
    lifted, tables, inc, full = refs[n:]
    inc[...] = jnp.zeros_like(inc)
    part_sum(0, group, t, chunks, lifted, tables, inc, full)


def begin_part(chunks, t, lifted, tables, group):
    count, lev, cells = lifted.shape
    out = (shape((SLOTS, lev, cells), F32), shape((count,) + chunks[0].shape[1:], chunks[0].dtype))
    return call(functools.partial(begin_kernel, len(chunks), group, t), out, [*chunks, lifted, tables])


def end_kernel(first, group, full_in, chunk, own, near, begun, lifted, tables, full, inc, half, acc):
    del full_in
    acc[...] = begun[...]
    if chunk is not None:
        part_sum(first, group, 2, [chunk], lifted, tables, acc, full)
    for t, part in enumerate((own, near, acc)):
        inc[t] = part[...]
        half[t] = part[...].astype(BF16)


def end_parts(chunk, own, near, begun, full, lifted, tables, group):
    count, lev, cells = lifted.shape
    field = (SLOTS, lev, cells)
    out = (shape(full.shape, full.dtype), shape((3,) + field, F32), shape((3,) + field, BF16))
    args = [full, chunk, own, near, begun, lifted, tables]
    kernel = functools.partial(end_kernel, count - chunk.shape[0], group)
    return call(kernel, out, args, [pltpu.VMEM(field, F32)], aliases={0: 0})


def columns(row, width):
    return jnp.broadcast_to(row.astype(F32), (width, row.shape[1])).T.astype(jnp.int32)


def lane_choice(column, start, width):
    lanes = lax.broadcasted_iota(jnp.int32, column.shape, 1)
    blocks = [jnp.where(column == lanes + (start + b), 1.0, 0.0).astype(BF16) for b in range(0, width, column.shape[1])]
    return blocks[0] if len(blocks) == 1 else jnp.concatenate(blocks, axis=1)


def row_choice(row, start, count):
    index = lax.broadcasted_iota(jnp.int32, (count, row.shape[1]), 0) + start
    return jnp.where(index == row, 1.0, 0.0).astype(BF16)


def code_rows(recv, rows):
    return [
        jnp.concatenate([recv[h, k : k + 1, :rows] for h in range(recv.shape[0])], axis=1) for k in range(6)
    ]


def selections(position, codes, weight, innov):
    half = codes[0].shape[1]
    column = columns(position, 128)
    pick = lane_choice(column, 0, 2 * half)
    pick_t = jnp.concatenate([row_choice(position, i * half, half) for i in range(2)], axis=1)
    onehot, onehot_t = [], []
    for t in range(3):
        pair = codes[2 * t : 2 * t + 2]
        onehot.append(jnp.concatenate([lane_choice(columns(row, 128), 0, CODES) for row in pair], axis=1))
        onehot_t.append(jnp.concatenate([row_choice(row, 0, CODES) for row in pair], axis=1))
    high = weight.astype(BF16)
    tiles = jnp.concatenate([high, (weight - high.astype(F32)).astype(BF16)], axis=2)
    turned = innov.T
    return pick, pick_t, onehot, onehot_t, tiles, jnp.concatenate([turned, turned], axis=1)


def selections_kernel(rows, position, codes, weight, innov, pick, pick_t, onehot, onehot_t, tiles, turned):
    obs = position.shape[1]
    member = lax.axis_index("member")
    kept = weight[pl.ds(member * (obs // TILE), obs // TILE)]
    seen = innov[:, pl.ds(pl.multiple_of(member * obs, obs), obs)]
    made = selections(position[0:1], code_rows(codes, rows), kept, seen)
    pick[...], pick_t[...] = made[0], made[1]
    for t in range(3):
        onehot[t], onehot_t[t] = made[2][t], made[3][t]
    tiles[...], turned[...] = made[4], made[5]


def select_all(rows, position, codes, weight, innov):
    obs = position.shape[1]
    half = codes.shape[0] * rows
    if rows % 16:
        member = lax.axis_index("member")
        kept = lax.dynamic_slice_in_dim(weight, member * (obs // TILE), obs // TILE, 0)
        seen = lax.dynamic_slice_in_dim(innov, member * obs, obs, 1)
        pick, pick_t, onehot, onehot_t, tiles, turned = selections(
            position[0:1], code_rows(codes, rows), kept, seen
        )
        return pick, pick_t, jnp.stack(onehot), jnp.stack(onehot_t), tiles, turned
    lev = innov.shape[0]
    out = (
        shape((obs, 2 * half), BF16),
        shape((half, 2 * obs), BF16),
        shape((3, half, 2 * CODES), BF16),
        shape((3, CODES, 2 * half), BF16),
        shape((obs // TILE, TILE, 2 * TILE), BF16),
        shape((obs, 2 * lev), F32),
    )
    return call(functools.partial(selections_kernel, rows), out, [position, codes, weight, innov])


def turn_kernel(group, sign, *refs):
    near, far, adj_own, adj_other, base, pert, tables, vert, vert_t, vec, inc, inc_half, square = refs[:13]
    adj, acc, moved, mixed = refs[13:]
    rows = vert.shape[0]
    lev = rows // group
    adj[...] = adj_own[...] + adj_other[...].astype(F32)
    acc[...] = jnp.zeros_like(acc)
    square[...] = jnp.zeros_like(square)
    sources = (pert, near, far)

    def project(g):
        parts = []
        for t in range(3):
            values = sources[t][pl.ds(g * group, group)].astype(F32)
            parts.append(
                jnp.concatenate(
                    [(values[j, 0] * adj[t, 0] + values[j, 1] * adj[t, 1]).astype(BF16) for j in range(group)],
                    axis=0,
                )
            )
        moved[g] = dot(jnp.concatenate(parts, axis=1), tables[...], ((1,), (1,))).astype(BF16)

    def lift(g):
        at = pl.ds(g * group, group)
        new = base[at].reshape(rows, CELLS) + dot(vert_t[...], moved[g])
        if sign < 0:
            new = -new
        vec[at] = new.reshape(group, lev, CELLS)
        if sign < 0:
            square[...] += jnp.sum((new * new).reshape(rows // 8, 8, CELLS), axis=0)

    def mix(g):
        half = vec[pl.ds(g * group, group)].reshape(rows, CELLS).astype(BF16)
        mixed[g] = dot(vert[...], half).astype(BF16)

    def gather(g):
        local = dot(mixed[g], tables[...])
        for t in range(3):
            values = sources[t][pl.ds(g * group, group)]
            for s in range(SLOTS):
                total = acc[t, s]
                for j in range(group):
                    part = local[j * lev : (j + 1) * lev, t * CELLS : (t + 1) * CELLS]
                    total += values[j, s].astype(F32) * part
                acc[t, s] = total

    stages = (gather, mix, lift, project)
    steps = base.shape[0] // group
    depth = len(stages)
    for i in range(min(depth - 1, steps)):
        for k, stage in enumerate(stages):
            if 0 <= i - (depth - 1 - k):
                stage(i - (depth - 1 - k))

    def step(g, _):
        for k, stage in enumerate(stages):
            stage(g - (depth - 1 - k))
        return 0

    lax.fori_loop(depth - 1, steps, step, 0)
    for i in range(max(steps, depth - 1), steps + depth - 1):
        for k, stage in enumerate(stages):
            if 0 <= i - (depth - 1 - k) < steps:
                stage(i - (depth - 1 - k))
    inc[...] = acc[...]
    inc_half[...] = acc[...].astype(BF16)


def turn(adj_own, adj_other, base, pert, near, far, tables, vert, vert_t, sign):
    count, lev, _ = base.shape
    group = vert.shape[0] // lev
    field = (3, SLOTS, lev, CELLS)
    out = (shape(base.shape, F32), shape(field, F32), shape(field, BF16), shape((8, CELLS), F32))
    half = pltpu.VMEM((count // group, group * lev, CELLS), BF16)
    return call(
        functools.partial(turn_kernel, group, sign),
        out,
        [near, far, adj_own, adj_other, base, pert, tables, vert, vert_t],
        [pltpu.VMEM(field, F32), pltpu.VMEM(field, F32), half, half],
    )


def three_pieces(row, rows):
    high = row.astype(BF16).astype(F32)
    mid = (row - high).astype(BF16).astype(F32)
    low = row - high - mid
    index = lax.broadcasted_iota(jnp.int32, (rows, row.shape[1]), 0)
    tile = jnp.where(index == 0, high, jnp.where(index == 1, mid, jnp.where(index == 2, low, 0.0)))
    return tile.astype(BF16)


def twice(cells):
    blank = jnp.zeros_like(cells)
    return jnp.concatenate(
        [jnp.concatenate([cells, blank], axis=1), jnp.concatenate([blank, cells], axis=1)], axis=0
    )


def scalar_row(values, width):
    lane = lax.broadcasted_iota(jnp.int32, (1, width), 1)
    row = jnp.zeros((1, width), F32)
    for i, value in enumerate(values):
        row = jnp.where(lane == i, value, row)
    return row


def sampled_rows(inc, other, onehot, t):
    total = (inc[t] + other[t].astype(F32)).astype(BF16)
    cells = jnp.concatenate([total[s] for s in range(SLOTS)], axis=1)
    return dot(onehot[t], twice(cells), ((1,), (1,))).astype(BF16)


def sample_kernel(regions, rows, kinds, inc, other, onehot, *refs):
    out = refs[-1]
    for t in range(kinds):
        found = sampled_rows(inc, other, onehot, t)
        for h in range(regions):
            out[h, t * rows : (t + 1) * rows] = found[h * rows : (h + 1) * rows]
    if len(refs) > 1:
        tile = three_pieces(scalar_row([jnp.sum(ref[...]) for ref in refs[:-1]], out.shape[2]), 8)
        for h in range(regions):
            out[h, kinds * rows :] = tile


def sample(regions, rows, inc, other, onehot, scal=()):
    kinds, lev = inc.shape[0], inc.shape[2]
    extra = 8 if scal else 0
    if rows % 16:
        parts = [sampled_rows(inc, other, onehot, t).reshape(regions, rows, 2 * lev) for t in range(kinds)]
        if scal:
            tile = three_pieces(scalar_row([jnp.sum(v) for v in scal], 2 * lev), 8)
            parts.append(jnp.broadcast_to(tile[None], (regions,) + tile.shape))
        return jnp.concatenate(parts, axis=1)
    return call(
        functools.partial(sample_kernel, regions, rows, kinds),
        shape((regions, kinds * rows + extra, 2 * lev), BF16),
        [inc, other, onehot, *scal],
    )


def gathered(regions, rows, kinds, recv):
    parts = []
    for e in range(regions):
        total = recv[e, 0:rows].astype(F32)
        for t in range(1, kinds):
            source = side(e, t, regions)
            if source is not None:
                total = total + recv[source, t * rows : (t + 1) * rows].astype(F32)
        parts.append(total)
    return jnp.concatenate(parts, axis=0)


def swap_lanes(values):
    half = values.shape[1] // 2
    return jnp.concatenate([values[:, half:], values[:, :half]], axis=1)


def departures(regions, rows, kinds, recv, pick):
    slots = gathered(regions, rows, kinds, recv)
    high = slots.astype(BF16).astype(F32)
    low = swap_lanes(slots - high)
    first = lax.broadcasted_iota(jnp.int32, slots.shape, 1) < slots.shape[1] // 2
    stacked = jnp.concatenate([jnp.where(first, high, low), jnp.where(first, low, high)], axis=0)
    found = dot(pick, stacked.astype(BF16))
    return found + swap_lanes(found)


def weigh(tiles, both):
    high = both.astype(BF16).astype(F32)
    first = lax.broadcasted_iota(jnp.int32, both.shape, 1) < both.shape[1] // 2
    split = jnp.where(first, high, both - high).astype(BF16)
    parts = []
    for i in range(tiles.shape[0]):
        own = split[i * TILE : (i + 1) * TILE]
        parts.append(dot(tiles[i], jnp.concatenate([own, own], axis=0)))
    out = jnp.concatenate(parts, axis=0)
    return out + swap_lanes(out)


def halves_apart(both):
    first = lax.broadcasted_iota(jnp.int32, both.shape, 1) < both.shape[1] // 2
    return jnp.concatenate([jnp.where(first, both, 0.0), jnp.where(first, 0.0, both)], axis=0).astype(BF16)


def column_sums(values):
    return jnp.sum(values.reshape(values.shape[0] // 8, 8, values.shape[1]), axis=0)


def weigh_kernel(regions, rows, kinds, recv, pick, pick_t, tiles, innov, out, dep_out, wgt_out, seen):
    dep = departures(regions, rows, kinds, recv, pick[...])
    if innov is not None:
        dep = dep - innov[...]
    wgt = weigh(tiles, dep)
    dep_out[...] = dep
    wgt_out[...] = wgt
    seen[...] = column_sums(0.5 * dep * wgt)
    back = dot(pick_t[...], halves_apart(wgt)).astype(BF16)
    for r in range(regions):
        for t in range(3):
            source = side(r, t, regions)
            if source is None:
                out[r, t * rows : (t + 1) * rows] = jnp.zeros((rows, back.shape[1]), BF16)
            else:
                out[r, t * rows : (t + 1) * rows] = back[source * rows : (source + 1) * rows]


def weigh_later_kernel(regions, rows, kinds, recv, pick, pick_t, tiles, out, dep_out, wgt_out, seen):
    weigh_kernel(regions, rows, kinds, recv, pick, pick_t, tiles, None, out, dep_out, wgt_out, seen)


def spread_regions(back, fill):
    regions = back.shape[0]
    tail = back.shape[1:]
    near = back.reshape((regions // 2, 2) + tail)[:, ::-1].reshape(back.shape)
    inner = back[1 : regions - 1].reshape((regions // 2 - 1, 2) + tail)[:, ::-1]
    blank = jnp.broadcast_to(fill, (1,) + tail)
    far = jnp.concatenate([blank, inner.reshape((regions - 2,) + tail), blank], axis=0)
    return jnp.concatenate([back, near, far], axis=1)


def weighed(regions, rows, recv, pick, pick_t, tiles, innov=None):
    lanes = recv.shape[2]
    kinds = recv.shape[1] // rows
    obs = pick.shape[0]
    if rows % 16:
        dep = departures(regions, rows, kinds, recv, pick)
        dep = dep if innov is None else dep - innov
        wgt = weigh(tiles, dep)
        back = dot(pick_t, halves_apart(wgt)).astype(BF16).reshape(regions, rows, lanes)
        return spread_regions(back, jnp.zeros((), BF16)), dep, wgt, column_sums(0.5 * dep * wgt)
    out = (
        shape((regions, 3 * rows, lanes), BF16),
        shape((obs, lanes), F32),
        shape((obs, lanes), F32),
        shape((8, lanes), F32),
    )
    args = [recv, pick, pick_t, tiles] + ([] if innov is None else [innov])
    kernel = weigh_later_kernel if innov is None else weigh_kernel
    return call(functools.partial(kernel, regions, rows, kinds), out, args)


def scattered_field(rows_t, onehot_t, lev):
    count = rows_t.shape[0]
    low = dot(onehot_t[:, :count], rows_t).T
    high = dot(onehot_t[:, count:], rows_t).T
    return low[:lev] + high[lev:]


def scatter_kernel(regions, rows, recv, onehot_t, out, half):
    lev = out.shape[2]
    for t in range(3):
        values = jnp.concatenate([recv[h, t * rows : (t + 1) * rows] for h in range(regions)], axis=0)
        field = scattered_field(values, onehot_t[t], lev)
        for s in range(SLOTS):
            piece = field[:, s * CELLS : (s + 1) * CELLS]
            out[t, s] = piece
            half[t, s] = piece.astype(BF16)


def scattered(regions, rows, recv, onehot_t):
    lanes = recv.shape[2]
    lev = lanes // 2
    if rows % 16:
        parts = []
        for t in range(3):
            values = recv[:, t * rows : (t + 1) * rows].reshape(regions * rows, lanes)
            field = scattered_field(values, onehot_t[t], lev)
            parts.append(jnp.stack([field[:, s * CELLS : (s + 1) * CELLS] for s in range(SLOTS)]))
        full = jnp.stack(parts)
        return full, full.astype(BF16)
    field = (3, SLOTS, lev, CELLS)
    return call(
        functools.partial(scatter_kernel, regions, rows),
        (shape(field, F32), shape(field, BF16)),
        [recv, onehot_t],
    )


def last_sums(regions, rows, recv, pick, tiles, dep, wgt, pieces, norms):
    total = jnp.sum(jnp.sum(pieces.astype(F32), axis=0), axis=0, keepdims=True)
    lane = lax.broadcasted_iota(jnp.int32, total.shape, 1)
    norm = jnp.sum(jnp.where(lane == 0, total, 0.0))
    seen = jnp.sum(jnp.where(lane == 1, total, 0.0))
    step = norm / (norm + seen)
    dep_image = departures(regions, rows, 3, recv, pick)
    dep_next = dep - step * dep_image
    wgt_next = weigh(tiles, dep_next)
    squares, mixed = norms(step)
    values = [
        squares,
        mixed,
        0.5 * jnp.sum(dep_next * wgt_next),
        0.5 * jnp.sum(dep_next * wgt),
    ]
    return scalar_row(values, 128), scalar_row([norm, seen, step], 128)


def last_kernel(regions, rows, group, recv, pick, tiles, dep, wgt, resid, image, out, known):
    count, lev, cells = resid.shape

    def norms(step):
        def add(g, carry):
            at = pl.ds(g * group, group)
            now = resid[at].reshape(group * lev, cells)
            later = now - step * image[at].reshape(group * lev, cells)
            return carry[0] + column_sums(later * later), carry[1] + column_sums(later * now)

        zero = jnp.zeros((8, cells), F32)
        squares, mixed = lax.fori_loop(0, count // group, add, (zero, zero))
        return jnp.sum(squares), jnp.sum(mixed)

    pieces = recv[:, 3 * rows : 3 * rows + 3]
    sums, facts = last_sums(regions, rows, recv, pick[...], tiles, dep[...], wgt[...], pieces, norms)
    wide = jnp.broadcast_to(sums, (8, 128))
    for r in range(regions):
        out[r] = wide
    known[...] = jnp.broadcast_to(facts, (8, 128))


def last(regions, rows, recv, pick, tiles, dep, wgt, resid, image):
    if rows % 16:

        def norms(step):
            later = resid - step * image
            return jnp.sum(later * later), jnp.sum(later * resid)

        sums, facts = last_sums(
            regions, rows, recv, pick, tiles, dep, wgt, recv[:, 3 * rows : 3 * rows + 3], norms
        )
        return jnp.broadcast_to(sums[None], (regions, 8, 128)), jnp.broadcast_to(facts, (8, 128))
    group = group_size(resid.shape[0])
    return call(
        functools.partial(last_kernel, regions, rows, group),
        (shape((regions, 8, 128), F32), shape((8, 128), F32)),
        [recv, pick, tiles, dep, wgt, resid, image],
    )


def finish(total, facts, emit):
    lane = lax.broadcasted_iota(jnp.int32, total.shape, 1)
    norm_next, mixed, seen_next, seen_mixed = (jnp.sum(jnp.where(lane == i, total, 0.0)) for i in range(4))
    norm, seen, step = (jnp.sum(jnp.where(lane == i, facts, 0.0)) for i in range(3))
    ratio = norm_next / norm
    curved = norm_next + seen_next + 2.0 * ratio * (mixed + seen_mixed) + ratio * ratio * (norm + seen)
    step_next = norm_next / curved
    along, across = step + step_next * (1.0 + ratio), step_next * step
    return emit(along, across)


def finish_kernel(group, sums, others, facts, control, resid, image, out):
    total = jnp.sum(sums[...] + others[...], axis=0)[0:1]

    def emit(along, across):
        def add(g, _):
            at = pl.ds(g * group, group)
            out[at] = control[at] + along * resid[at] - across * image[at]
            return 0

        lax.fori_loop(0, control.shape[0] // group, add, 0)

    finish(total, facts[0:1], emit)


def finished(sums, others, facts, control, resid, image):
    group = group_size(control.shape[0])
    return call(
        functools.partial(finish_kernel, group),
        jax.ShapeDtypeStruct(control.shape, F32),
        [sums, others, facts, control, resid, image],
    )


def to_regions(values):
    return lax.all_to_all(values, "region", split_axis=0, concat_axis=0, tiled=True)


def other_members(own, half):
    if lax.axis_size("member") == 2:
        return own, lax.ppermute(half, "member", [(0, 1), (1, 0)])
    return lax.psum(half, "member").astype(F32), jnp.zeros_like(half)


def member_sum(values):
    if lax.axis_size("member") == 2:
        return values + lax.ppermute(values, "member", [(0, 1), (1, 0)])
    return lax.psum(values, "member")


def local(
    perturbations,
    control,
    vertical_loc,
    block_kernels,
    loc_pattern,
    obs_region,
    obs_slot,
    obs_cell,
    innovations,
    obs_weight,
):
    regions = lax.axis_size("region")
    members = lax.axis_size("member")
    member = lax.axis_index("member")
    count, _, _ = control.shape
    obs = obs_region.shape[0] // members
    cap = max(2, 2 * obs // regions)

    group = group_size(count)
    sizes = halo_sizes(count // group)
    starts = [sum(sizes[:i]) * group for i in range(len(sizes) + 1)]
    rest = lax.optimization_barrier(perturbations)
    pieces = [(rest if i else perturbations)[starts[i] : starts[i + 1]] for i in range(len(sizes))]
    near_p, far_p = halo(pieces)

    first = member * obs
    targets = lax.dynamic_slice_in_dim(obs_region[:, 0], first, obs, 0)
    codes = lax.dynamic_slice_in_dim(obs_slot * CELLS + obs_cell, first, obs, 0)
    named = targets[:, None] == jnp.arange(regions, dtype=jnp.int32)[None, :]
    lower = lax.broadcasted_iota(jnp.int32, (obs, obs), 0) > lax.broadcasted_iota(jnp.int32, (obs, obs), 1)
    earlier = dot(lower.astype(BF16), named.astype(BF16))
    rank = jnp.sum(jnp.where(named, earlier, 0.0), axis=1).astype(jnp.int32)
    rows = cap // 2
    slots_of_half = regions * rows
    position = (rank // rows) * slots_of_half + targets * rows + rank % rows
    slots = jnp.arange(2 * slots_of_half, dtype=jnp.int32)
    slot_codes = dot((slots[:, None] == position[None, :]).astype(BF16), (codes + 1).astype(BF16)[:, None])
    slot_codes = slot_codes[:, 0].astype(jnp.int32) - 1
    slot_codes = slot_codes.reshape(2, regions, rows).transpose(1, 0, 2)
    sent_codes = spread_regions(slot_codes, jnp.full((), -1, jnp.int32))
    sent_codes = jnp.pad(sent_codes, ((0, 0), (0, 2), (0, 128 - rows)))
    got_codes = to_regions(sent_codes)
    spots = jnp.broadcast_to(position[None], (8, obs))
    got_codes, loc_pattern = lax.optimization_barrier((got_codes, loc_pattern))
    pick, pick_t, onehot, onehot_t, tiles, innov = select_all(
        rows, spots, got_codes, obs_weight, innovations
    )
    pick, far_p[-2] = lax.optimization_barrier((pick, far_p[-2]))

    own, lifted, tables, vert, vert_t = own_forward(
        loc_pattern.T, control, perturbations, block_kernels, vertical_loc, group
    )
    near, near_p = begin_part(near_p, 1, lifted, tables, group)
    begun, joined = begin_part(far_p[:-1], 2, lifted, tables, group)
    far_p, inc, half = end_parts(far_p[-1], own, near, begun, joined, lifted, tables, group)
    inc, other = other_members(inc, half)
    recv = to_regions(sample(regions, rows, inc, other, onehot))
    back, _, _, _ = weighed(regions, rows, recv, pick, pick_t, tiles, innov)
    adj, adj_half = scattered(regions, rows, to_regions(back), onehot_t)
    adj, adj_other = other_members(adj, adj_half)
    resid, inc, half, square = turn(
        adj, adj_other, control, perturbations, near_p, far_p, tables, vert, vert_t, -1
    )

    inc, other = other_members(inc, half)
    recv = to_regions(sample(regions, rows, inc, other, onehot))
    back, dep, wgt, seen = weighed(regions, rows, recv, pick, pick_t, tiles)
    adj, adj_half = scattered(regions, rows, to_regions(back), onehot_t)
    adj, adj_other = other_members(adj, adj_half)
    square, seen = member_sum(square), member_sum(seen)
    image, inc, half, _ = turn(
        adj, adj_other, resid, perturbations, near_p, far_p, tables, vert, vert_t, 1
    )

    inc, other = other_members(inc, half)
    recv = to_regions(sample(regions, rows, inc, other, onehot, (square, seen)))
    sums, facts = last(regions, rows, recv, pick, tiles, dep, wgt, resid, image)
    sums, others = other_members(*[to_regions(sums)] * 2)
    return finished(sums, others, facts, control, resid, image)


def solution(mesh):
    placed = (
        P("member", None, None, "region"),
        P("member", None, "region"),
        P(),
        P(),
        P(),
        P("region", None),
        P("region"),
        P("region"),
        P(None, "region"),
        P("region", None, None),
    )

    return jax.shard_map(local, mesh=mesh, in_specs=placed, out_specs=P("member", None, "region"), check_vma=False)
```

```python
import functools

import jax
import jax.numpy as jnp
from jax import lax
from jax.experimental import pallas as pl
from jax.experimental.pallas import tpu as pltpu
from jax.sharding import PartitionSpec as P


SLOTS = 2
TILE = 128
CELLS = 128
CODES = SLOTS * CELLS
F32 = jnp.float32
BF16 = jnp.bfloat16
HALO_SHARES = (3, 3, 2, 2)


def near_of(r):
    return r ^ 1


def far_of(r, regions):
    other = r - 1 if r % 2 == 0 else r + 1
    return other if 0 <= other < regions else None


def side(r, t, regions):
    return (r, near_of(r), far_of(r, regions))[t]


def dot(a, b, dims=((1,), (0,)), precision=None):
    return lax.dot_general(a, b, (dims, ((), ())), precision=precision, preferred_element_type=F32)


def halo(chunks):
    regions = lax.axis_size("region")
    pairs = [(r, r ^ 1) for r in range(regions)]
    onward = [(r, r + 2 if r % 2 == 0 else r - 2) for r in range(regions)]
    onward = [(s, d) for s, d in onward if 0 <= d < regions]
    near, far = [], []
    for chunk in chunks:
        near.append(lax.ppermute(chunk, "region", pairs))
    for chunk in near:
        far.append(lax.ppermute(chunk, "region", onward))
    return near, far


def call(kernel, out_shape, args, scratch=(), limit=16, scalars=(), aliases=None):
    vmem = pl.BlockSpec(memory_space=pltpu.VMEM)
    return pl.pallas_call(
        kernel,
        out_shape=out_shape,
        in_specs=[pl.BlockSpec(memory_space=pltpu.SMEM)] * len(scalars) + [vmem] * len(args),
        out_specs=jax.tree.map(lambda _: vmem, out_shape),
        scratch_shapes=list(scratch),
        input_output_aliases=aliases or {},
        compiler_params=pltpu.CompilerParams(vmem_limit_bytes=limit << 20),
    )(*scalars, *[pltpu.with_memory_space_constraint(a, pltpu.VMEM) for a in args])


def halo_sizes(groups):
    whole = sum(HALO_SHARES)
    ends = sorted({max(1, groups * sum(HALO_SHARES[: i + 1]) // whole) for i in range(len(HALO_SHARES))})
    if len(ends) < 2:
        ends = [1, groups]
    return [b - a for a, b in zip([0] + ends, ends)]


def group_size(members):
    return 4 if members % 4 == 0 else 2 if members % 2 == 0 else 1


def shape(dims, dtype):
    return pltpu.VMEM(dims, dtype)


def block_diagonal(matrix, copies, transposed):
    side_by_side = jnp.concatenate([matrix] * copies, axis=0)
    size, total = matrix.shape[0], copies * matrix.shape[0]
    index = lax.broadcasted_iota(jnp.int32, (size, total), 0)
    lane = lax.broadcasted_iota(jnp.int32, (size, total), 1)
    parts = []
    for i in range(copies):
        place = (lane == index + i * size).astype(BF16)
        part = side_by_side[i * size : (i + 1) * size]
        parts.append(dot(part, place, ((0 if transposed else 1,), (0,))).astype(BF16))
    return jnp.concatenate(parts, axis=0)


def own_kernel(group, pattern, start, pert, kernels, vloc, inc, lifted, tables, vert, vert_t):
    count, lev, _ = start.shape
    rows = group * lev
    vert[...] = block_diagonal(vloc[...], group, False)
    vert_t[...] = block_diagonal(vloc[...], group, True)
    region = lax.axis_index("region")
    even = region % 2 == 0
    up = pattern[0, jnp.minimum(region + 1, pattern.shape[1] - 1)]
    down = pattern[2, jnp.maximum(region - 1, 0)]
    picks = (pattern[1, region], jnp.where(even, up, down), jnp.where(even, down, up))
    for t in range(3):
        tables[:, t * CELLS : (t + 1) * CELLS] = kernels[picks[t]]

    def mix(g):
        at = pl.ds(g * group, group)
        mixed = dot(vert[...], start[at].reshape(rows, CELLS).astype(BF16)).astype(BF16)
        lifted[at] = mixed.reshape(group, lev, CELLS)

    def gather(g):
        at = pl.ds(g * group, group)
        local = dot(lifted[at].reshape(rows, CELLS), tables[:, :CELLS])
        values = pert[at]
        for s in range(SLOTS):
            for j in range(group):
                totals[s] = totals[s] + values[j, s].astype(F32) * local[j * lev : (j + 1) * lev]

    steps = count // group
    totals = [jnp.zeros((lev, CELLS), F32)] * SLOTS
    mix(0)
    for g in range(1, steps):
        mix(g)
        gather(g - 1)
    gather(steps - 1)
    for s in range(SLOTS):
        inc[s] = totals[s]


def own_forward(pattern, start, pert, kernels, vloc, group):
    _, lev, _ = start.shape
    field = (SLOTS, lev, CELLS)
    square = shape((group * lev, group * lev), BF16)
    out = (shape(field, F32), shape(start.shape, BF16), shape((CELLS, 3 * CELLS), BF16), square, square)
    return call(
        functools.partial(own_kernel, group),
        out,
        [start, pert, kernels, vloc],
        scalars=[pattern],
    )


def part_sum(first, group, t, chunks, lifted, tables, acc, full):
    lev = lifted.shape[1]
    rows = group * lev
    totals = [acc[s] for s in range(SLOTS)]
    for chunk in chunks:
        for g in range(chunk.shape[0] // group):
            at = slice(first + g * group, first + (g + 1) * group)
            local = dot(lifted[at].reshape(rows, CELLS), tables[:, t * CELLS : (t + 1) * CELLS])
            values = chunk[g * group : (g + 1) * group]
            full[at] = values
            for s in range(SLOTS):
                for j in range(group):
                    totals[s] = totals[s] + values[j, s].astype(F32) * local[j * lev : (j + 1) * lev]
        first += chunk.shape[0]
    for s in range(SLOTS):
        acc[s] = totals[s]


def begin_kernel(n, group, t, *refs):
    chunks = refs[:n]
    lifted, tables, inc, full = refs[n:]
    inc[...] = jnp.zeros_like(inc)
    part_sum(0, group, t, chunks, lifted, tables, inc, full)


def begin_part(chunks, t, lifted, tables, group):
    count, lev, cells = lifted.shape
    out = (shape((SLOTS, lev, cells), F32), shape((count,) + chunks[0].shape[1:], chunks[0].dtype))
    return call(functools.partial(begin_kernel, len(chunks), group, t), out, [*chunks, lifted, tables])


def end_kernel(first, group, full_in, chunk, own, near, begun, lifted, tables, full, inc, half, acc):
    del full_in
    acc[...] = begun[...]
    if chunk is not None:
        part_sum(first, group, 2, [chunk], lifted, tables, acc, full)
    for t, part in enumerate((own, near, acc)):
        inc[t] = part[...]
        half[t] = part[...].astype(BF16)


def end_parts(chunk, own, near, begun, full, lifted, tables, group):
    count, lev, cells = lifted.shape
    field = (SLOTS, lev, cells)
    out = (shape(full.shape, full.dtype), shape((3,) + field, F32), shape((3,) + field, BF16))
    args = [full, chunk, own, near, begun, lifted, tables]
    kernel = functools.partial(end_kernel, count - chunk.shape[0], group)
    return call(kernel, out, args, [pltpu.VMEM(field, F32)], aliases={0: 0})


def columns(row, width):
    return jnp.broadcast_to(row.astype(F32), (width, row.shape[1])).T.astype(jnp.int32)


def lane_choice(column, start, width):
    lanes = lax.broadcasted_iota(jnp.int32, column.shape, 1)
    blocks = [jnp.where(column == lanes + (start + b), 1.0, 0.0).astype(BF16) for b in range(0, width, column.shape[1])]
    return blocks[0] if len(blocks) == 1 else jnp.concatenate(blocks, axis=1)


def row_choice(row, start, count):
    index = lax.broadcasted_iota(jnp.int32, (count, row.shape[1]), 0) + start
    return jnp.where(index == row, 1.0, 0.0).astype(BF16)


def code_rows(recv, rows):
    return [
        jnp.concatenate([recv[h, k : k + 1, :rows] for h in range(recv.shape[0])], axis=1) for k in range(6)
    ]


def selections(position, codes, weight, innov):
    half = codes[0].shape[1]
    column = columns(position, 128)
    pick = lane_choice(column, 0, 2 * half)
    pick_t = jnp.concatenate([row_choice(position, i * half, half) for i in range(2)], axis=1)
    onehot, onehot_t = [], []
    for t in range(3):
        pair = codes[2 * t : 2 * t + 2]
        onehot.append(jnp.concatenate([lane_choice(columns(row, 128), 0, CODES) for row in pair], axis=1))
        onehot_t.append(jnp.concatenate([row_choice(row, 0, CODES) for row in pair], axis=1))
    high = weight.astype(BF16)
    tiles = jnp.concatenate([high, (weight - high.astype(F32)).astype(BF16)], axis=2)
    turned = innov.T
    return pick, pick_t, onehot, onehot_t, tiles, jnp.concatenate([turned, turned], axis=1)


def selections_kernel(rows, position, codes, weight, innov, pick, pick_t, onehot, onehot_t, tiles, turned):
    obs = position.shape[1]
    member = lax.axis_index("member")
    kept = weight[pl.ds(member * (obs // TILE), obs // TILE)]
    seen = innov[:, pl.ds(pl.multiple_of(member * obs, obs), obs)]
    made = selections(position[0:1], code_rows(codes, rows), kept, seen)
    pick[...], pick_t[...] = made[0], made[1]
    for t in range(3):
        onehot[t], onehot_t[t] = made[2][t], made[3][t]
    tiles[...], turned[...] = made[4], made[5]


def select_all(rows, position, codes, weight, innov):
    obs = position.shape[1]
    half = codes.shape[0] * rows
    if rows % 16:
        member = lax.axis_index("member")
        kept = lax.dynamic_slice_in_dim(weight, member * (obs // TILE), obs // TILE, 0)
        seen = lax.dynamic_slice_in_dim(innov, member * obs, obs, 1)
        pick, pick_t, onehot, onehot_t, tiles, turned = selections(
            position[0:1], code_rows(codes, rows), kept, seen
        )
        return pick, pick_t, jnp.stack(onehot), jnp.stack(onehot_t), tiles, turned
    lev = innov.shape[0]
    out = (
        shape((obs, 2 * half), BF16),
        shape((half, 2 * obs), BF16),
        shape((3, half, 2 * CODES), BF16),
        shape((3, CODES, 2 * half), BF16),
        shape((obs // TILE, TILE, 2 * TILE), BF16),
        shape((obs, 2 * lev), F32),
    )
    return call(functools.partial(selections_kernel, rows), out, [position, codes, weight, innov])


def turn_kernel(group, sign, *refs):
    near, far, adj_own, adj_other, base, pert, tables, vert, vert_t, vec, inc, inc_half, square = refs[:13]
    adj, acc, moved, mixed = refs[13:]
    rows = vert.shape[0]
    lev = rows // group
    adj[...] = adj_own[...] + adj_other[...].astype(F32)
    acc[...] = jnp.zeros_like(acc)
    square[...] = jnp.zeros_like(square)
    sources = (pert, near, far)

    def project(g):
        parts = []
        for t in range(3):
            values = sources[t][pl.ds(g * group, group)].astype(F32)
            parts.append(
                jnp.concatenate(
                    [(values[j, 0] * adj[t, 0] + values[j, 1] * adj[t, 1]).astype(BF16) for j in range(group)],
                    axis=0,
                )
            )
        moved[g] = dot(jnp.concatenate(parts, axis=1), tables[...], ((1,), (1,))).astype(BF16)

    def lift(g):
        at = pl.ds(g * group, group)
        new = base[at].reshape(rows, CELLS) + dot(vert_t[...], moved[g])
        if sign < 0:
            new = -new
        vec[at] = new.reshape(group, lev, CELLS)
        if sign < 0:
            square[...] += jnp.sum((new * new).reshape(rows // 8, 8, CELLS), axis=0)

    def mix(g):
        half = vec[pl.ds(g * group, group)].reshape(rows, CELLS).astype(BF16)
        mixed[g] = dot(vert[...], half).astype(BF16)

    def gather(g):
        local = dot(mixed[g], tables[...])
        for t in range(3):
            values = sources[t][pl.ds(g * group, group)]
            for s in range(SLOTS):
                total = acc[t, s]
                for j in range(group):
                    part = local[j * lev : (j + 1) * lev, t * CELLS : (t + 1) * CELLS]
                    total += values[j, s].astype(F32) * part
                acc[t, s] = total

    stages = (gather, mix, lift, project)
    steps = base.shape[0] // group
    depth = len(stages)
    for i in range(min(depth - 1, steps)):
        for k, stage in enumerate(stages):
            if 0 <= i - (depth - 1 - k):
                stage(i - (depth - 1 - k))

    def step(g, _):
        for k, stage in enumerate(stages):
            stage(g - (depth - 1 - k))
        return 0

    lax.fori_loop(depth - 1, steps, step, 0)
    for i in range(max(steps, depth - 1), steps + depth - 1):
        for k, stage in enumerate(stages):
            if 0 <= i - (depth - 1 - k) < steps:
                stage(i - (depth - 1 - k))
    inc[...] = acc[...]
    inc_half[...] = acc[...].astype(BF16)


def turn(adj_own, adj_other, base, pert, near, far, tables, vert, vert_t, sign):
    count, lev, _ = base.shape
    group = vert.shape[0] // lev
    field = (3, SLOTS, lev, CELLS)
    out = (shape(base.shape, F32), shape(field, F32), shape(field, BF16), shape((8, CELLS), F32))
    half = pltpu.VMEM((count // group, group * lev, CELLS), BF16)
    return call(
        functools.partial(turn_kernel, group, sign),
        out,
        [near, far, adj_own, adj_other, base, pert, tables, vert, vert_t],
        [pltpu.VMEM(field, F32), pltpu.VMEM(field, F32), half, half],
    )


def piece_rows(sums, width):
    rows = []
    for value in sums:
        high = value.astype(BF16).astype(F32)
        mid = (value - high).astype(BF16).astype(F32)
        rows += [high, mid, value - high - mid]
    index = lax.broadcasted_iota(jnp.int32, (8, width), 0)
    tile = jnp.zeros((8, width), F32)
    for i, row in enumerate(rows):
        tile = jnp.where(index == i, row, tile)
    return tile.astype(BF16)


def full_sum(values):
    return jnp.sum(jnp.sum(values, axis=0, keepdims=True), axis=1, keepdims=True)


def twice(cells):
    blank = jnp.zeros_like(cells)
    return jnp.concatenate(
        [jnp.concatenate([cells, blank], axis=1), jnp.concatenate([blank, cells], axis=1)], axis=0
    )


def row_tile(rows, width):
    index = lax.broadcasted_iota(jnp.int32, (8, width), 0)
    tile = jnp.zeros((8, width), F32)
    for i, row in enumerate(rows):
        tile = jnp.where(index == i, row, tile)
    return tile


def sampled_rows(inc, other, onehot, t):
    total = (inc[t] + other[t].astype(F32)).astype(BF16)
    cells = jnp.concatenate([total[s] for s in range(SLOTS)], axis=1)
    return dot(onehot[t], twice(cells), ((1,), (1,))).astype(BF16)


def sample_kernel(regions, rows, kinds, inc, other, onehot, *refs):
    out = refs[-1]
    for t in range(kinds):
        found = sampled_rows(inc, other, onehot, t)
        for h in range(regions):
            out[h, t * rows : (t + 1) * rows] = found[h * rows : (h + 1) * rows]
    if len(refs) > 1:
        tile = piece_rows([full_sum(ref[...]) for ref in refs[:-1]], out.shape[2])
        for h in range(regions):
            out[h, kinds * rows :] = tile


def sample(regions, rows, inc, other, onehot, scal=()):
    kinds, lev = inc.shape[0], inc.shape[2]
    extra = 8 if scal else 0
    if rows % 16:
        parts = [sampled_rows(inc, other, onehot, t).reshape(regions, rows, 2 * lev) for t in range(kinds)]
        if scal:
            tile = piece_rows([full_sum(v) for v in scal], 2 * lev)
            parts.append(jnp.broadcast_to(tile[None], (regions,) + tile.shape))
        return jnp.concatenate(parts, axis=1)
    return call(
        functools.partial(sample_kernel, regions, rows, kinds),
        shape((regions, kinds * rows + extra, 2 * lev), BF16),
        [inc, other, onehot, *scal],
    )


def gathered(regions, rows, kinds, recv):
    parts = []
    for e in range(regions):
        total = recv[e, 0:rows].astype(F32)
        for t in range(1, kinds):
            source = side(e, t, regions)
            if source is not None:
                total = total + recv[source, t * rows : (t + 1) * rows].astype(F32)
        parts.append(total)
    return jnp.concatenate(parts, axis=0)


def swap_lanes(values):
    half = values.shape[1] // 2
    return jnp.concatenate([values[:, half:], values[:, :half]], axis=1)


def departures(regions, rows, kinds, recv, pick):
    slots = gathered(regions, rows, kinds, recv)
    high = slots.astype(BF16).astype(F32)
    low = swap_lanes(slots - high)
    first = lax.broadcasted_iota(jnp.int32, slots.shape, 1) < slots.shape[1] // 2
    stacked = jnp.concatenate([jnp.where(first, high, low), jnp.where(first, low, high)], axis=0)
    found = dot(pick, stacked.astype(BF16))
    return found + swap_lanes(found)


def weigh(tiles, both):
    high = both.astype(BF16).astype(F32)
    first = lax.broadcasted_iota(jnp.int32, both.shape, 1) < both.shape[1] // 2
    split = jnp.where(first, high, both - high).astype(BF16)
    parts = []
    for i in range(tiles.shape[0]):
        own = split[i * TILE : (i + 1) * TILE]
        parts.append(dot(tiles[i], jnp.concatenate([own, own], axis=0)))
    out = jnp.concatenate(parts, axis=0)
    return out + swap_lanes(out)


def halves_apart(both):
    first = lax.broadcasted_iota(jnp.int32, both.shape, 1) < both.shape[1] // 2
    return jnp.concatenate([jnp.where(first, both, 0.0), jnp.where(first, 0.0, both)], axis=0).astype(BF16)


def column_sums(values):
    return jnp.sum(values.reshape(values.shape[0] // 8, 8, values.shape[1]), axis=0)


def weigh_kernel(regions, rows, kinds, recv, pick, pick_t, tiles, innov, out, dep_out, wgt_out, seen):
    dep = departures(regions, rows, kinds, recv, pick[...])
    if innov is not None:
        dep = dep - innov[...]
    wgt = weigh(tiles, dep)
    dep_out[...] = dep
    wgt_out[...] = wgt
    seen[...] = column_sums(0.5 * dep * wgt)
    back = dot(pick_t[...], halves_apart(wgt)).astype(BF16)
    for r in range(regions):
        for t in range(3):
            source = side(r, t, regions)
            if source is None:
                out[r, t * rows : (t + 1) * rows] = jnp.zeros((rows, back.shape[1]), BF16)
            else:
                out[r, t * rows : (t + 1) * rows] = back[source * rows : (source + 1) * rows]


def weigh_later_kernel(regions, rows, kinds, recv, pick, pick_t, tiles, out, dep_out, wgt_out, seen):
    weigh_kernel(regions, rows, kinds, recv, pick, pick_t, tiles, None, out, dep_out, wgt_out, seen)


def spread_regions(back, fill):
    regions = back.shape[0]
    tail = back.shape[1:]
    near = back.reshape((regions // 2, 2) + tail)[:, ::-1].reshape(back.shape)
    inner = back[1 : regions - 1].reshape((regions // 2 - 1, 2) + tail)[:, ::-1]
    blank = jnp.broadcast_to(fill, (1,) + tail)
    far = jnp.concatenate([blank, inner.reshape((regions - 2,) + tail), blank], axis=0)
    return jnp.concatenate([back, near, far], axis=1)


def weighed(regions, rows, recv, pick, pick_t, tiles, innov=None):
    lanes = recv.shape[2]
    kinds = recv.shape[1] // rows
    obs = pick.shape[0]
    if rows % 16:
        dep = departures(regions, rows, kinds, recv, pick)
        dep = dep if innov is None else dep - innov
        wgt = weigh(tiles, dep)
        back = dot(pick_t, halves_apart(wgt)).astype(BF16).reshape(regions, rows, lanes)
        return spread_regions(back, jnp.zeros((), BF16)), dep, wgt, column_sums(0.5 * dep * wgt)
    out = (
        shape((regions, 3 * rows, lanes), BF16),
        shape((obs, lanes), F32),
        shape((obs, lanes), F32),
        shape((8, lanes), F32),
    )
    args = [recv, pick, pick_t, tiles] + ([] if innov is None else [innov])
    kernel = weigh_later_kernel if innov is None else weigh_kernel
    return call(functools.partial(kernel, regions, rows, kinds), out, args)


def scattered_field(rows_t, onehot_t, lev):
    count = rows_t.shape[0]
    low = dot(onehot_t[:, :count], rows_t).T
    high = dot(onehot_t[:, count:], rows_t).T
    return low[:lev] + high[lev:]


def scatter_kernel(regions, rows, recv, onehot_t, out, half):
    lev = out.shape[2]
    for t in range(3):
        values = jnp.concatenate([recv[h, t * rows : (t + 1) * rows] for h in range(regions)], axis=0)
        field = scattered_field(values, onehot_t[t], lev)
        for s in range(SLOTS):
            piece = field[:, s * CELLS : (s + 1) * CELLS]
            out[t, s] = piece
            half[t, s] = piece.astype(BF16)


def scattered(regions, rows, recv, onehot_t):
    lanes = recv.shape[2]
    lev = lanes // 2
    if rows % 16:
        parts = []
        for t in range(3):
            values = recv[:, t * rows : (t + 1) * rows].reshape(regions * rows, lanes)
            field = scattered_field(values, onehot_t[t], lev)
            parts.append(jnp.stack([field[:, s * CELLS : (s + 1) * CELLS] for s in range(SLOTS)]))
        full = jnp.stack(parts)
        return full, full.astype(BF16)
    field = (3, SLOTS, lev, CELLS)
    return call(
        functools.partial(scatter_kernel, regions, rows),
        (shape(field, F32), shape(field, BF16)),
        [recv, onehot_t],
    )


def last_sums(regions, rows, recv, pick, tiles, dep, wgt, pieces, norms):
    total = jnp.sum(pieces.astype(F32), axis=0)
    norm, seen = jnp.sum(total[0:3], axis=0, keepdims=True), jnp.sum(total[3:6], axis=0, keepdims=True)
    step = norm / (norm + seen)
    dep_image = departures(regions, rows, 3, recv, pick)
    dep_next = dep - step * dep_image
    wgt_next = weigh(tiles, dep_next)
    squares, mixed = norms(step)
    values = [
        squares,
        mixed,
        full_sum(0.5 * column_sums(dep_next * wgt_next)),
        full_sum(0.5 * column_sums(dep_next * wgt)),
    ]
    return row_tile(values, 128), row_tile([norm, seen, step], 128)


def last_kernel(regions, rows, group, recv, pick, tiles, dep, wgt, resid, image, out, known):
    count, lev, cells = resid.shape

    def norms(step):
        def add(g, carry):
            at = pl.ds(g * group, group)
            now = resid[at].reshape(group * lev, cells)
            later = now - step * image[at].reshape(group * lev, cells)
            return carry[0] + column_sums(later * later), carry[1] + column_sums(later * now)

        zero = jnp.zeros((8, cells), F32)
        squares, mixed = lax.fori_loop(0, count // group, add, (zero, zero), unroll=count // group)
        return full_sum(squares), full_sum(mixed)

    pieces = recv[:, 3 * rows :]
    sums, facts = last_sums(regions, rows, recv, pick[...], tiles, dep[...], wgt[...], pieces, norms)
    for r in range(regions):
        out[r] = sums
    known[...] = facts


def last(regions, rows, recv, pick, tiles, dep, wgt, resid, image):
    if rows % 16:

        def norms(step):
            later = resid - step * image
            return full_sum(jnp.sum(later * later, axis=0)), full_sum(jnp.sum(later * resid, axis=0))

        sums, facts = last_sums(
            regions, rows, recv, pick, tiles, dep, wgt, recv[:, 3 * rows :], norms
        )
        return jnp.broadcast_to(sums[None], (regions, 8, 128)), facts
    group = group_size(resid.shape[0])
    return call(
        functools.partial(last_kernel, regions, rows, group),
        (shape((regions, 8, 128), F32), shape((8, 128), F32)),
        [recv, pick, tiles, dep, wgt, resid, image],
    )


def finish_kernel(group, sums, others, facts, control, resid, image, out):
    total = jnp.sum(sums[...] + others[...], axis=0)
    norm_next, mixed, seen_next, seen_mixed = (total[i : i + 1] for i in range(4))
    norm, seen, step = (facts[i : i + 1] for i in range(3))
    ratio = norm_next / norm
    curved = norm_next + seen_next + 2.0 * ratio * (mixed + seen_mixed) + ratio * ratio * (norm + seen)
    step_next = norm_next / curved
    rows = group * control.shape[1]
    along = jnp.broadcast_to(step + step_next * (1.0 + ratio), (rows, CELLS))
    across = jnp.broadcast_to(step_next * step, (rows, CELLS))
    for g in range(control.shape[0] // group):
        at = slice(g * group, (g + 1) * group)
        new = (
            control[at].reshape(rows, CELLS)
            + along * resid[at].reshape(rows, CELLS)
            - across * image[at].reshape(rows, CELLS)
        )
        out[at] = new.reshape(group, control.shape[1], CELLS)


def finished(sums, others, facts, control, resid, image):
    group = group_size(control.shape[0])
    return call(
        functools.partial(finish_kernel, group),
        jax.ShapeDtypeStruct(control.shape, F32),
        [sums, others, facts, control, resid, image],
    )


def to_regions(values):
    return lax.all_to_all(values, "region", split_axis=0, concat_axis=0, tiled=True)


def other_members(own, half):
    if lax.axis_size("member") == 2:
        return own, lax.ppermute(half, "member", [(0, 1), (1, 0)])
    return lax.psum(half, "member").astype(F32), jnp.zeros_like(half)


def member_sum(values):
    if lax.axis_size("member") == 2:
        return values + lax.ppermute(values, "member", [(0, 1), (1, 0)])
    return lax.psum(values, "member")


def local(
    perturbations,
    control,
    vertical_loc,
    block_kernels,
    loc_pattern,
    obs_region,
    obs_slot,
    obs_cell,
    innovations,
    obs_weight,
):
    regions = lax.axis_size("region")
    members = lax.axis_size("member")
    member = lax.axis_index("member")
    count, _, _ = control.shape
    obs = obs_region.shape[0] // members
    cap = max(2, 2 * obs // regions)

    group = group_size(count)
    sizes = halo_sizes(count // group)
    starts = [sum(sizes[:i]) * group for i in range(len(sizes) + 1)]
    rest = lax.optimization_barrier(perturbations)
    pieces = [(rest if i else perturbations)[starts[i] : starts[i + 1]] for i in range(len(sizes))]
    near_p, far_p = halo(pieces)

    first = member * obs
    targets = lax.dynamic_slice_in_dim(obs_region[:, 0], first, obs, 0)
    codes = lax.dynamic_slice_in_dim(obs_slot * CELLS + obs_cell, first, obs, 0)
    named = targets[:, None] == jnp.arange(regions, dtype=jnp.int32)[None, :]
    lower = lax.broadcasted_iota(jnp.int32, (obs, obs), 0) > lax.broadcasted_iota(jnp.int32, (obs, obs), 1)
    earlier = dot(lower.astype(BF16), named.astype(BF16))
    rank = jnp.sum(jnp.where(named, earlier, 0.0), axis=1).astype(jnp.int32)
    rows = cap // 2
    slots_of_half = regions * rows
    position = (rank // rows) * slots_of_half + targets * rows + rank % rows
    slots = jnp.arange(2 * slots_of_half, dtype=jnp.int32)
    slot_codes = dot((slots[:, None] == position[None, :]).astype(BF16), (codes + 1).astype(BF16)[:, None])
    slot_codes = slot_codes[:, 0].astype(jnp.int32) - 1
    slot_codes = slot_codes.reshape(2, regions, rows).transpose(1, 0, 2)
    sent_codes = spread_regions(slot_codes, jnp.full((), -1, jnp.int32))
    sent_codes = jnp.pad(sent_codes, ((0, 0), (0, 2), (0, 128 - rows)))
    got_codes = to_regions(sent_codes)
    spots = jnp.broadcast_to(position[None], (8, obs))
    got_codes, loc_pattern = lax.optimization_barrier((got_codes, loc_pattern))
    pick, pick_t, onehot, onehot_t, tiles, innov = select_all(
        rows, spots, got_codes, obs_weight, innovations
    )
    pick, far_p[-2] = lax.optimization_barrier((pick, far_p[-2]))

    own, lifted, tables, vert, vert_t = own_forward(
        loc_pattern.T, control, perturbations, block_kernels, vertical_loc, group
    )
    near, near_p = begin_part(near_p, 1, lifted, tables, group)
    begun, joined = begin_part(far_p[:-1], 2, lifted, tables, group)
    far_p, inc, half = end_parts(far_p[-1], own, near, begun, joined, lifted, tables, group)
    inc, other = other_members(inc, half)
    recv = to_regions(sample(regions, rows, inc, other, onehot))
    back, _, _, _ = weighed(regions, rows, recv, pick, pick_t, tiles, innov)
    adj, adj_half = scattered(regions, rows, to_regions(back), onehot_t)
    adj, adj_other = other_members(adj, adj_half)
    resid, inc, half, square = turn(
        adj, adj_other, control, perturbations, near_p, far_p, tables, vert, vert_t, -1
    )

    inc, other = other_members(inc, half)
    recv = to_regions(sample(regions, rows, inc, other, onehot))
    back, dep, wgt, seen = weighed(regions, rows, recv, pick, pick_t, tiles)
    adj, adj_half = scattered(regions, rows, to_regions(back), onehot_t)
    adj, adj_other = other_members(adj, adj_half)
    square, seen = member_sum(square), member_sum(seen)
    image, inc, half, _ = turn(
        adj, adj_other, resid, perturbations, near_p, far_p, tables, vert, vert_t, 1
    )

    inc, other = other_members(inc, half)
    recv = to_regions(sample(regions, rows, inc, other, onehot, (square, seen)))
    sums, facts = last(regions, rows, recv, pick, tiles, dep, wgt, resid, image)
    sums, others = other_members(*[to_regions(sums)] * 2)
    return finished(sums, others, facts, control, resid, image)


def solution(mesh):
    placed = (
        P("member", None, None, "region"),
        P("member", None, "region"),
        P(),
        P(),
        P(),
        P("region", None),
        P("region"),
        P("region"),
        P(None, "region"),
        P("region", None, None),
    )

    return jax.shard_map(local, mesh=mesh, in_specs=placed, out_specs=P("member", None, "region"), check_vma=False)
```
